32 devices in a mesh: dp: 4 (over x, y), tp: 8 (over z, core).
Axes of the slice: x: 2, y: 2, z: 4, core: 2. Of those that a mesh axis runs over, the one named last changes fastest.
Arguments:
- x: bfloat16 [4096, 8192], P(('dp', 'tp')), parts along dimension 0
- gain_a: bfloat16 [8192], replicated
- wq: bfloat16 [8192, 8192], P(None, 'tp')
- wk: bfloat16 [8192, 8192], P(None, 'tp')
- wv: bfloat16 [8192, 8192], P(None, 'tp')
- wo: bfloat16 [8192, 8192], P('tp')
- gain_m: bfloat16 [8192], replicated
- w_gate: bfloat16 [8192, 24576], P(None, 'tp')
- w_up: bfloat16 [8192, 24576], P(None, 'tp')
- w_down: bfloat16 [24576, 8192], P('tp')
Outputs:
- output: bfloat16 [4096, 8192], P(('dp', 'tp')), parts along dimension 0
There are 4 independent parts. The reference program is written for one: setup_inputs(seed, part) draws one part's arguments, and reference() takes and returns one part's arrays. A program takes and returns all parts, laid end to end along the dimension named above; an argument that names none is the same for every part.
All inputs are finite; a program needn't handle non-finite values.
Results may differ from the reference program's by a relative error of at most 0.017.
Values are sent between devices in bfloat16 or wider.
A program may use at most 2 GiB of HBM per device.

```python
import jax
import jax.numpy as jnp
from jax import lax

ROWS = 1024
D = 8192
HEADS = 64
KV_HEADS = 64
HEAD = 128
FF = 24576
THETA = 10000


def setup_inputs(seed: int = 0, part: int = 0) -> dict:
    kx, kn, kq, kk, kv, ko, km, kg, ku, kd = jax.random.split(jax.random.key(seed), 10)

    def weights(key, rows, columns):
        return jax.random.normal(key, (rows, columns), jnp.float32) * rows**-0.5

    drawn = {
        "x": jax.random.normal(jax.random.fold_in(kx, part), (ROWS, D), jnp.float32),
        "gain_a": 1 + 0.1 * jax.random.normal(kn, (D,), jnp.float32),
        "wq": 2 * weights(kq, D, HEADS * HEAD),
        "wk": 2 * weights(kk, D, KV_HEADS * HEAD),
        "wv": 4 * weights(kv, D, KV_HEADS * HEAD),
        "wo": weights(ko, HEADS * HEAD, D),
        "gain_m": 1 + 0.1 * jax.random.normal(km, (D,), jnp.float32),
        "w_gate": weights(kg, D, FF),
        "w_up": weights(ku, D, FF),
        "w_down": 2 * weights(kd, FF, D),
    }
    return {k: v.astype(jnp.bfloat16) for k, v in drawn.items()}


def normed(x, gain):
    wide = x.astype(jnp.float32)
    scale = lax.rsqrt(jnp.mean(wide * wide, -1, keepdims=True) + 1e-6)
    return (wide * scale * gain.astype(jnp.float32)).astype(jnp.bfloat16)


def turned(t, place, theta):
    half = t.shape[-1] // 2
    angle = place.astype(jnp.float32)[:, None] * theta ** (-jnp.arange(half, dtype=jnp.float32) / half)
    cos, sin = jnp.cos(angle)[:, None], jnp.sin(angle)[:, None]
    a, b = t[..., :half].astype(jnp.float32), t[..., half:].astype(jnp.float32)
    return jnp.concatenate([a * cos - b * sin, b * cos + a * sin], -1).astype(jnp.bfloat16)


def matmul(a, w):
    return jnp.dot(a, w, preferred_element_type=jnp.float32).astype(jnp.bfloat16)


def einsum(form, a, b):
    return jnp.einsum(form, a.astype(jnp.float32), b.astype(jnp.float32))


def attention(q, k, v):
    scores = einsum("tgsd,ugd->gstu", q, k) * q.shape[-1] ** -0.5
    token = jnp.arange(q.shape[0])
    scores = jnp.where(token[:, None] >= token, scores, -jnp.inf)
    weights = jax.nn.softmax(scores, -1).astype(jnp.bfloat16)
    return einsum("gstu,ugd->tgsd", weights, v).astype(jnp.bfloat16)


def reference(x, gain_a, wq, wk, wv, wo, gain_m, w_gate, w_up, w_down):
    a, place = normed(x, gain_a), jnp.arange(ROWS)
    q = turned(matmul(a, wq).reshape(ROWS, HEADS, HEAD), place, THETA).reshape(ROWS, KV_HEADS, -1, HEAD)
    k = turned(matmul(a, wk).reshape(ROWS, KV_HEADS, HEAD), place, THETA)
    v = matmul(a, wv).reshape(ROWS, KV_HEADS, HEAD)
    seen = attention(q, k, v).reshape(ROWS, HEADS * HEAD)
    h = (x.astype(jnp.float32) + jnp.dot(seen, wo, preferred_element_type=jnp.float32)).astype(jnp.bfloat16)
    b = normed(h, gain_m)
    gate = jnp.dot(b, w_gate, preferred_element_type=jnp.float32)
    up = jnp.dot(b, w_up, preferred_element_type=jnp.float32)
    hidden = (jax.nn.silu(gate) * up).astype(jnp.bfloat16)
    return (h.astype(jnp.float32) + jnp.dot(hidden, w_down, preferred_element_type=jnp.float32)).astype(jnp.bfloat16)
```

```python
import functools

import jax
import jax.numpy as jnp
from jax import lax
from jax.experimental import pallas as pl
from jax.experimental.pallas import tpu as pltpu
from jax.sharding import PartitionSpec as P

HEAD = 128
THETA = 10000
LOG2E = 1.4426950408889634
D = 8192
R = 128
HALF = R // 2
W = 512
NT = D // W
SLOTS = 3
MID = 3072
QKV_TILES = MID // W
GU_TILES = MID // (W // 2)
PASSES = 4
LAG_OPP, LAG_END = 3, 5
ACCS = LAG_END + 1
MESH = pl.DeviceIdType.MESH
F32, BF16 = jnp.float32, jnp.bfloat16


def _dot(a, b):
    return jnp.dot(a, b, preferred_element_type=F32)


def _kernel(x_ref, ga_ref, gm_ref, wq, wk, wv, wo, wg, wu, wd, y_ref,
            xf, mid, wbuf, acc, sd, so, sn, res, cosb, sinb,
            ld_sem, w_sem, ag_s, ag_r, d2_s, d2_r, sd_s, so_s, sn_s, rd, ro, rn, out_sem, ready):
    dp, tp = lax.axis_index("dp"), lax.axis_index("tp")
    z, c = lax.div(tp, 2), lax.rem(tp, 2)
    zm, zp, zo = lax.rem(z + 3, 4), lax.rem(z + 1, 4), lax.rem(z + 2, 4)
    partner, left, right = (dp, 2 * z + 1 - c), (dp, 2 * zm + c), (dp, 2 * zp + c)
    own = 2 * z + c
    peers = (partner, left, right)

    def greet(sem):
        for peer in peers:
            pl.semaphore_signal(sem, inc=1, device_id=peer, device_id_type=MESH)

    def cols(t, width):
        return pl.ds(pl.multiple_of(t * width, width), width)

    def qkv_copy(t, slot, w):
        return pltpu.make_async_copy(w.at[:, cols(lax.rem(t, 2), W)], wbuf.at[slot], w_sem.at[slot])

    def fetch_qkv(t, slot):
        for n, w in enumerate((wq, wk, wv)):
            @pl.when(lax.div(t, 2) == n)
            def _():
                qkv_copy(t, slot, w).start()

    def gu_copies(t, slot):
        return [pltpu.make_async_copy(w.at[:, cols(t, W // 2)], wbuf.at[slot, :, pl.ds(n * (W // 2), W // 2)], w_sem.at[slot])
                for n, w in enumerate((wg, wu))]

    def fetch_gu(t, slot):
        for copy in gu_copies(t, slot):
            copy.start()

    def down_copy(w, j, slot):
        return pltpu.make_async_copy(w.at[:, cols(j, W)], wbuf.at[slot, pl.ds(0, w.shape[0]), :], w_sem.at[slot])

    def piece(side, msg):
        zz = zo if msg == 2 else (zm, zp)[side]
        half = (side, 1 - side, side)[msg]
        return xf.at[2 * zz + c, pl.ds(half * HALF, HALF), :]

    def send(side, msg):
        if msg == 2:
            ref = piece(1 - side, 0)
        else:
            half = (1 - side, side)[msg]
            ref = xf.at[own, pl.ds(half * HALF, HALF), :]
        return pltpu.make_async_remote_copy(ref, ref, ag_s.at[side, msg], ag_r.at[1 - side, msg], device_id=(left, right)[side],
                                            device_id_type=MESH)

    def landed(side, msg):
        ref = piece(side, msg)
        return pltpu.make_async_remote_copy(ref, ref, ag_s.at[side, msg], ag_r.at[side, msg], device_id=(left, right)[side],
                                            device_id_type=MESH)

    def across(n, ref):
        return pltpu.make_async_remote_copy(ref, ref, d2_s.at[n], d2_r.at[n], device_id=partner, device_id_type=MESH)

    def across_own():
        return across(0, xf.at[own])

    def across_piece(side, msg):
        return across(1 + side * 3 + msg, piece(side, msg))

    def other(side, msg):
        zz = zo if msg == 2 else (zm, zp)[side]
        half = (side, 1 - side, side)[msg]
        return across(1 + side * 3 + msg, xf.at[2 * zz + 1 - c, pl.ds(half * HALF, HALF), :])

    def gather_start():
        across_own().start()
        for msg in range(2):
            for side in range(2):
                send(side, msg).start()

    def arrive(msg):
        for side in range(2):
            landed(side, msg).wait_recv()
            if msg == 0:
                send(1 - side, 2).start()
            across_piece(side, msg).start()

    def arrive_other(msg):
        for side in range(2):
            other(side, msg).wait_recv()

    def gather_end():
        across_own().wait_send()
        for msg in range(3):
            for side in range(2):
                send(side, msg).wait_send()
                across_piece(side, msg).wait_send()

    def granules(p):
        mids = (p == 1) | (p == 2)
        out = []
        for lane in range(2):
            for s in range(2):
                zz = jnp.where(p == 0, z, jnp.where(mids, (zm, zp)[s], zo))
                half = jnp.where(p == 2, 1 - s, s)
                out.append((2 * zz + lane, half))
        return out

    def rows_of(half):
        return pl.ds(pl.multiple_of(half * HALF, HALF), HALF)

    def events(s, per):
        for msg in range(3):
            @pl.when(s == (msg + 1) * per - 1)
            def _():
                pass

            @pl.when(s == (msg + 1) * per)
            def _():
                arrive(msg)
                arrive_other(msg)

    def normed(src, gain_ref):
        def body(i, _):
            rows = pl.ds(pl.multiple_of(i * 16, 16), 16)
            wide = src[rows, :].astype(F32)
            scale = lax.rsqrt(jnp.mean(wide * wide, -1, keepdims=True) + 1e-6)
            xf[own, rows, :] = (wide * scale * gain_ref[...].astype(F32)).astype(BF16)
            return 0
        lax.fori_loop(0, R // 16, body, 0)

    def scatter(k, w, base, after, ready_sem, write):
        here = 0
        for_lane = lambda lane: jnp.concatenate([mid[2 * zz + lane, :, :k] for zz in range(4)], axis=0)

        def to_partner(j, slot):
            return pltpu.make_async_remote_copy(sd.at[slot], xf.at[pl.ds(0, 4), :, cols(j, W)], sd_s.at[slot], rd.at[j], device_id=partner,
                                                device_id_type=MESH)

        def to_side_opp(side, j, slot):
            return pltpu.make_async_remote_copy(so.at[slot, pl.ds(side * HALF, HALF), :],
                                                xf.at[4, pl.ds(side * HALF, HALF), cols(j, W)],
                                                so_s.at[side, slot], ro.at[side, j], device_id=(left, right)[side], device_id_type=MESH)

        def half_of(side, part):
            return side if part == 0 else 1 - side

        def to_side(side, part, j, slot):
            rows = pl.ds(half_of(side, part) * HALF, HALF)
            return pltpu.make_async_remote_copy(sn.at[slot, side, rows, :], xf.at[5 + side, rows, cols(j, W)],
                                                sn_s.at[side, part, slot], rn.at[side, part, j], device_id=(left, right)[side],
                                                device_id_type=MESH)

        def step(j, dots, full):
            def when(cond):
                return (lambda f: f()) if full else pl.when(cond)

            j1, j3, j5 = j - 1, j - LAG_OPP, j - LAG_END
            if dots:
                down_copy(w, j, lax.rem(base + j, SLOTS)).wait()
                @when(j >= 2)
                def _():
                    to_partner(j - 2, lax.rem(j, 2)).wait_send()
            @when((j1 >= 0) & (j1 < NT))
            def _():
                to_partner(j1, lax.rem(j1, 2)).wait_recv()
                @when(j1 >= 2)
                def _():
                    for side in range(2):
                        to_side_opp(side, j1 - 2, lax.rem(j1, 2)).wait_send()
                        to_side(side, 1, j1 - 2, lax.rem(j1, 2)).wait_send()
            @when((j3 >= 0) & (j3 < NT))
            def _():
                for side in range(2):
                    to_side_opp(side, j3, 0).wait_recv()
                @when(j3 >= 2)
                def _():
                    for side in range(2):
                        to_side(side, 0, j3 - 2, lax.rem(j3, 2)).wait_send()
            @when((j5 >= 0) & (j5 < NT))
            def _():
                for side in range(2):
                    for part in range(2):
                        to_side(side, part, j5, 0).wait_recv()
            if dots:
                after(j)
            @when((j5 >= 0) & (j5 < NT))
            def _():
                a = lax.rem(j5, ACCS)
                res[:, cols(j5, W)] = (res[:, cols(j5, W)].astype(F32)
                                       + (acc[a, z] + xf[5, :, cols(j5, W)].astype(F32) + xf[6, :, cols(j5, W)].astype(F32))).astype(BF16)
            @when((j3 >= 0) & (j3 < NT))
            def _():
                a = lax.rem(j3, ACCS)
                for side in range(2):
                    rows = pl.ds(side * HALF, HALF)
                    sn[lax.rem(j3, 2), side, rows, :] = (acc[a, (zm, zp)[side], rows, :] + xf[4, rows, cols(j3, W)].astype(F32)).astype(BF16)
            @when((j1 >= 0) & (j1 < NT))
            def _():
                a, slot = lax.rem(j1, ACCS), lax.rem(j1, 2)
                so[slot] = (acc[a, zo] + xf[zo, :, cols(j1, W)].astype(F32)).astype(BF16)
                for side in range(2):
                    zz = (zm, zp)[side]
                    rows, keep = pl.ds((1 - side) * HALF, HALF), pl.ds(side * HALF, HALF)
                    sn[slot, side, rows, :] = (acc[a, zz, rows, :] + xf[zz, rows, cols(j1, W)].astype(F32)).astype(BF16)
                    acc[a, zz, keep, :] = acc[a, zz, keep, :] + xf[zz, keep, cols(j1, W)].astype(F32)
                acc[a, z] = acc[a, z] + xf[z, :, cols(j1, W)].astype(F32)
            if dots:
                tile = wbuf[lax.rem(base + j, SLOTS), :k, :]
                sd[lax.rem(j, 2)] = _dot(for_lane(1 - c), tile).astype(BF16).reshape(4, R, W)
                acc[lax.rem(j, ACCS)] = _dot(for_lane(c), tile).reshape(4, R, W)
            if dots and not full:
                @pl.when(j == 0)
                def _():
                    pl.semaphore_wait(ready_sem, 3)
            @when((j1 >= 0) & (j1 < NT))
            def _():
                for side in range(2):
                    to_side_opp(side, j1, lax.rem(j1, 2)).start()
                    to_side(side, 1, j1, lax.rem(j1, 2)).start()
            @when((j3 >= 0) & (j3 < NT))
            def _():
                for side in range(2):
                    to_side(side, 0, j3, lax.rem(j3, 2)).start()
            if dots:
                to_partner(j, lax.rem(j, 2)).start()
            if write:
                @when((j5 >= 0) & (j5 < NT))
                def _():
                    pltpu.make_async_copy(res.at[:, cols(j5, W)], y_ref.at[:, cols(j5, W)], out_sem).start()
            return 0

        lax.fori_loop(0, LAG_END, lambda j, _: step(j, True, False), 0)
        lax.fori_loop(LAG_END, NT, lambda j, _: step(j, True, True), 0)
        lax.fori_loop(NT, NT + LAG_END, lambda j, _: step(j, False, False), 0)
        for j in (NT - 2, NT - 1):
            to_partner(j, j % 2).wait_send()
            for side in range(2):
                to_side_opp(side, j, j % 2).wait_send()
                for part in range(2):
                    to_side(side, part, j, j % 2).wait_send()

    greet(pltpu.get_barrier_semaphore())
    pltpu.make_async_copy(x_ref, res, ld_sem).start()
    g0 = 0
    for s in range(2):
        fetch_qkv(jnp.int32(s), s)
    pltpu.make_async_copy(x_ref, res, ld_sem).wait()
    normed(res, ga_ref)
    pl.semaphore_wait(pltpu.get_barrier_semaphore(), 3)
    gather_start()

    def table(i, _):
        rows = pl.ds(pl.multiple_of(i * R, R), R)
        lane = lax.broadcasted_iota(jnp.int32, (R, HEAD), 1)
        place = (i * R + lax.broadcasted_iota(jnp.int32, (R, HEAD), 0)).astype(F32)
        low = lane < HEAD // 2
        power = -jnp.where(low, lane, lane - HEAD // 2).astype(F32) / (HEAD // 2)
        angle = place * jnp.exp(power * jnp.float32(9.210340371976184))
        cosb[rows, :] = jnp.cos(angle)
        sinb[rows, :] = jnp.where(low, -1.0, 1.0) * jnp.sin(angle)
        return 0
    lax.fori_loop(0, 8, table, 0)
    across_own().wait_recv()

    steps1 = PASSES * QKV_TILES

    def qkv_step(s, _):
        events(s, QKV_TILES)
        slot = lax.rem(s, SLOTS)
        p, t = lax.div(s, QKV_TILES), lax.rem(s, QKV_TILES)
        qkv_copy(t, slot, wq).wait()
        nxt = lax.rem(s + 2, SLOTS)
        @pl.when(s + 2 < steps1)
        def _():
            fetch_qkv(lax.rem(s + 2, QKV_TILES), nxt)
        @pl.when(s + 2 >= steps1)
        def _():
            down_copy(wo, s + 2 - steps1, nxt).start()
        parts = granules(p)
        lhs = jnp.concatenate([xf[b, rows_of(h), :] for b, h in parts], axis=0)
        got = _dot(lhs, wbuf[slot]).astype(BF16).astype(F32)
        plain = t >= 4
        places = [pl.ds(pl.multiple_of(b * R + h * HALF, HALF), HALF) for b, h in parts]
        cos = jnp.where(plain, 1.0, jnp.concatenate([cosb[r, :] for r in places], axis=0))
        sin = jnp.where(plain, 0.0, jnp.concatenate([sinb[r, :] for r in places], axis=0))
        for n in range(W // HEAD):
            one = got[:, n * HEAD : (n + 1) * HEAD]
            out = (one * cos + pltpu.roll(one, HEAD // 2, 1) * sin).astype(BF16)
            for i, (b, h) in enumerate(parts):
                mid[b, rows_of(h), pl.ds(pl.multiple_of(t * W + n * HEAD, HEAD), HEAD)] = out[i * HALF : (i + 1) * HALF]
        return 0

    lax.fori_loop(0, steps1, qkv_step, 0)
    gather_end()
    greet(ready.at[0])

    e = HEAD**-0.5 * LOG2E

    def head(h, _):
        qc = pl.ds(pl.multiple_of(h * HEAD, HEAD), HEAD)
        kc = pl.ds(pl.multiple_of(h * HEAD + 1024, HEAD), HEAD)
        vc = pl.ds(pl.multiple_of(h * HEAD + 2048, HEAD), HEAD)
        for i in range(4):
            n = 256 * (i + 1)
            q = mid[2 * i : 2 * i + 2, :, qc].reshape(256, HEAD)
            k = mid[0 : 2 * i + 2, :, kc].reshape(n, HEAD)
            v = mid[0 : 2 * i + 2, :, vc].reshape(n, HEAD)
            s = lax.dot_general(q, k, (((1,), (1,)), ((), ())), preferred_element_type=F32)
            last = s[:, n - 256 :]
            seen = lax.broadcasted_iota(jnp.int32, (256, 256), 0) >= lax.broadcasted_iota(jnp.int32, (256, 256), 1)
            last = jnp.where(seen, last, -1e30)
            s = jnp.concatenate([s[:, : n - 256], last], axis=1) if i else last
            top = jnp.max(s, axis=1, keepdims=True)
            p = jnp.exp2((s - top) * e).astype(BF16)
            o = _dot(p, jnp.concatenate([v, jnp.ones((n, HEAD), BF16)], axis=1))
            mid[2 * i : 2 * i + 2, :, qc] = (o[:, :HEAD] / o[:, HEAD:]).astype(BF16).reshape(2, R, HEAD)
        return 0
    lax.fori_loop(0, 8, head, 0)

    def after_o(j):
        nxt = lax.rem(steps1 + j + 2, SLOTS)
        @pl.when(j + 2 < NT)
        def _():
            down_copy(wo, j + 2, nxt).start()
        @pl.when(j + 2 >= NT)
        def _():
            fetch_gu(j + 2 - NT, nxt)
    scatter(1024, wo, steps1, after_o, ready.at[0], False)
    greet(ready.at[1])

    base = steps1 + NT
    normed(res, gm_ref)
    pl.semaphore_wait(ready.at[1], 3)
    gather_start()
    across_own().wait_recv()
    steps2 = PASSES * GU_TILES

    def gu_step(s, _):
        events(s, GU_TILES)
        slot = lax.rem(base + s, SLOTS)
        p, t = lax.div(s, GU_TILES), lax.rem(s, GU_TILES)
        for copy in gu_copies(t, slot):
            copy.wait()
        nxt = lax.rem(base + s + 2, SLOTS)
        @pl.when(s + 2 < steps2)
        def _():
            fetch_gu(lax.rem(s + 2, GU_TILES), nxt)
        @pl.when(s + 2 >= steps2)
        def _():
            down_copy(wd, s + 2 - steps2, nxt).start()
        parts = granules(p)
        lhs = jnp.concatenate([xf[b, rows_of(h), :] for b, h in parts], axis=0)
        gate = _dot(lhs, wbuf[slot, :, : W // 2])
        up = _dot(lhs, wbuf[slot, :, W // 2 :])
        out = (gate * jax.nn.sigmoid(gate) * up).astype(BF16)
        for i, (b, h) in enumerate(parts):
            mid[b, rows_of(h), cols(t, W // 2)] = out[i * HALF : (i + 1) * HALF]
        return 0
    lax.fori_loop(0, steps2, gu_step, 0)
    gather_end()
    greet(ready.at[2])

    base2 = base + steps2

    def after_d(j):
        @pl.when(j + 2 < NT)
        def _():
            down_copy(wd, j + 2, lax.rem(base2 + j + 2, SLOTS)).start()
    scatter(MID, wd, base2, after_d, ready.at[2], True)
    pltpu.make_async_copy(res, y_ref, out_sem).wait()


def _layer(x, gain_a, wq, wk, wv, wo, gain_m, w_gate, w_up, w_down):
    hbm, vmem = pl.BlockSpec(memory_space=pl.ANY), pl.BlockSpec(memory_space=pltpu.VMEM)
    dma = pltpu.SemaphoreType.DMA
    return pl.pallas_call(
        _kernel,
        out_shape=jax.ShapeDtypeStruct((R, D), BF16),
        in_specs=[hbm, vmem, vmem] + [hbm] * 7,
        out_specs=hbm,
        scratch_shapes=[
            pltpu.VMEM((8, R, D), BF16),
            pltpu.VMEM((8, R, MID), BF16),
            pltpu.VMEM((SLOTS, D, W), BF16),
            pltpu.VMEM((ACCS, 4, R, W), F32),
            pltpu.VMEM((2, 4, R, W), BF16),
            pltpu.VMEM((2, R, W), BF16),
            pltpu.VMEM((2, 2, R, W), BF16),
            pltpu.VMEM((R, D), BF16),
            pltpu.VMEM((8 * R, HEAD), F32),
            pltpu.VMEM((8 * R, HEAD), F32),
            dma, dma((SLOTS,)),
            dma((2, 3)), dma((2, 3)), dma((7,)), dma((7,)),
            dma((2,)), dma((2, 2)), dma((2, 2, 2)), dma((NT,)), dma((2, NT)), dma((2, 2, NT)),
            dma, pltpu.SemaphoreType.REGULAR((3,)),
        ],
        compiler_params=pltpu.CompilerParams(collective_id=0, has_side_effects=True, vmem_limit_bytes=67043328),
    )(x, gain_a.reshape(1, D), gain_m.reshape(1, D), wq, wk, wv, wo, w_gate, w_up, w_down)


def solution(mesh):
    tokens, columns, rows_of = P(("dp", "tp"), None), P(None, "tp"), P("tp", None)
    return jax.shard_map(
        _layer,
        mesh=mesh,
        in_specs=(tokens, P(None), columns, columns, columns, rows_of, P(None), columns, columns, rows_of),
        out_specs=tokens,
        check_vma=False,
    )
```

```python
import functools

import jax
import jax.numpy as jnp
from jax import lax
from jax.experimental import pallas as pl
from jax.experimental.pallas import tpu as pltpu
from jax.sharding import PartitionSpec as P

HEAD = 128
LOG2E = 1.4426950408889634
LOG_THETA = 9.210340371976184
D = 8192
R = 128
C = 2 * R
PIECES = 4
PR = R // PIECES
W = 512
T = 512
NT = D // T
HIDDEN = 3072
QKV_STEPS, GU_STEPS, DOWN_STEPS = 12, 12, 8
RING, SENDS = 8, 4
LAG = 4
LATE, LAG_DOWN, HELD = 8, 5, 24
MESH = pl.DeviceIdType.MESH
F32, BF16 = jnp.float32, jnp.bfloat16


def _dot(a, b):
    return jnp.dot(a, b, preferred_element_type=F32)


def _kernel(x_ref, ga_ref, gm_ref, wq, wk, wv, wo, wg, wu, wd, y_ref,
            xf, wbuf, pend, res, d2buf, hid, st, sdb, ring, sbuf, cosb, sinb,
            ld_sem, w_sem, ag_s, ag_r, gd_s, gd_r, own_s, own_r, t_s, t_r, s_s, s_r, credit, d2free, ready):
    dp, tp = lax.axis_index("dp"), lax.axis_index("tp")
    z, c = lax.div(tp, 2), lax.rem(tp, 2)
    up_z, down_z = jnp.minimum(z + 1, 3), jnp.maximum(z - 1, 0)
    partner, above, below = (dp, 2 * z + 1 - c), (dp, 2 * up_z + c), (dp, 2 * down_z + c)
    own = 2 * z + c
    n_peers = 1 + jnp.minimum(z, 1) + jnp.minimum(3 - z, 1)

    def remote(src, dst, send_sem, recv_sem, to):
        return pltpu.make_async_remote_copy(src, dst, send_sem, recv_sem, device_id=to, device_id_type=MESH)

    def signal(sem, to):
        pl.semaphore_signal(sem, inc=1, device_id=to, device_id_type=MESH)

    def greet(sem):
        signal(sem, partner)
        @pl.when(z < 3)
        def _():
            signal(sem, above)
        @pl.when(z > 0)
        def _():
            signal(sem, below)

    def cols(t, width):
        return pl.ds(pl.multiple_of(t * width, width), width)

    def qkv_tile(t):
        return wbuf.at[lax.rem(lax.div(t, 2), 2), :, cols(lax.rem(t, 2), W // 2)]

    def qkv_copy(t, w):
        return pltpu.make_async_copy(w.at[:, cols(lax.rem(t, 4), W // 2)], qkv_tile(t), w_sem.at[lax.rem(t, 4)])

    def fetch_qkv(t):
        for n, w in enumerate((wq, wk, wv)):
            @pl.when(lax.div(t, 4) == n)
            def _():
                qkv_copy(t, w).start()

    def out_copies(half):
        return [pltpu.make_async_copy(wo.at[:, (8 * half + n) * T : (8 * half + n + 1) * T], wbuf.at[half, n * 1024 : (n + 1) * 1024, :],
                                      w_sem.at[half]) for n in range(8)]

    def fetch_out(half):
        for copy in out_copies(half):
            copy.start()

    def gu_copies(t, slot):
        return [pltpu.make_async_copy(w.at[:, cols(t, W // 2)], wbuf.at[slot, :, pl.ds(n * (W // 2), W // 2)], w_sem.at[slot])
                for n, w in enumerate((wg, wu))]

    def fetch_gu(t, slot):
        for copy in gu_copies(t, slot):
            copy.start()

    def down_copies(w, s, slot):
        k = w.shape[0]
        return [pltpu.make_async_copy(w.at[:, cols(2 * s + n, W)], wbuf.at[slot, pl.ds(n * k, k), :], w_sem.at[slot]) for n in range(2)]

    def fetch_down(w, s, slot):
        for copy in down_copies(w, s, slot):
            copy.start()

    def gather(causal):
        beats = (PIECES * z, PIECES * (3 - z))
        hop = (1 if causal else PIECES, PIECES)
        to = (above, below)
        can = (z < 3, z > 0)

        def place(dir, b):
            if dir == 1:
                chunk, piece = z + 1 + lax.div(b, PIECES), lax.rem(b, PIECES)
            elif not causal:
                chunk, piece = z - 1 - lax.div(b, PIECES), lax.rem(b, PIECES)
            else:
                o = b - (z - 1)
                later = jnp.maximum(o - PIECES, 0)
                chunk = jnp.where(o < 0, z - 1 - b, jnp.where(o < PIECES, 0, 1 + lax.div(later, PIECES - 1)))
                piece = jnp.where(o < 0, 0, jnp.where(o < PIECES, o, 1 + lax.rem(later, PIECES - 1)))
            return chunk, pl.ds(pl.multiple_of(piece * PR, PR), PR)

        def at(dir, b, lane):
            chunk, rows = place(dir, b)
            return xf.at[2 * chunk + lane, rows, :]

        def send(dir, ref, b):
            return remote(ref, ref, ag_s.at[dir, b], ag_r.at[dir, b], to[dir])

        def send_own(dir, piece, b):
            ref = xf.at[own, pl.ds(piece * PR, PR), :]
            @pl.when(can[dir])
            def _():
                send(dir, ref, b).start()

        def across(dir, b, lane):
            ref = at(dir, b, lane)
            return remote(ref, ref, gd_s.at[dir, b], gd_r.at[dir, b], partner)

        def across_own(lane):
            ref = xf.at[2 * z + lane]
            return remote(ref, ref, own_s, own_r, partner)

        def start():
            across_own(c).start()
            for piece in range(PIECES):
                send_own(1, piece, piece)
                if not causal:
                    send_own(0, piece, piece)
            if causal:
                send_own(0, 0, 0)
                @pl.when(z == 0)
                def _():
                    for piece in range(1, PIECES):
                        send_own(0, piece, piece)

        def event(b):
            for dir in range(2):
                @pl.when(b < beats[dir])
                def _():
                    ref = at(dir, b, c)
                    send(dir, ref, b).wait_recv()
                    @pl.when(can[dir])
                    def _():
                        send(dir, ref, b + hop[dir]).start()
                    across(dir, b, c).start()
                    if dir == 0 and causal:
                        @pl.when(b == beats[0] - 1)
                        def _():
                            for piece in range(1, PIECES):
                                send_own(0, piece, PIECES * z + piece)

        def events(a, b):
            lax.fori_loop(a, b, lambda i, _: (event(i), 0)[1], 0)

        def landed(a, b):
            def body(i, _):
                for dir in range(2):
                    @pl.when(i < beats[dir])
                    def _():
                        across(dir, i, 1 - c).wait_recv()
                return 0
            lax.fori_loop(a, b, body, 0)

        def landed_own():
            across_own(1 - c).wait_recv()

        def end():
            across_own(c).wait_send()
            for dir in range(2):
                def sent(i, _):
                    send(dir, xf.at[own, pl.ds(0, PR), :], i).wait_send()
                    return 0
                @pl.when(can[dir])
                def _():
                    lax.fori_loop(0, beats[dir] + PIECES, sent, 0)
                def crossed(i, _):
                    across(dir, i, c).wait_send()
                    return 0
                lax.fori_loop(0, beats[dir], crossed, 0)

        return start, event, events, landed, landed_own, end

    def side_of(d, causal):
        if not causal:
            return jnp.where(d > z, 0, 1)
        k = jnp.where(d < z, d + 1, d)
        return jnp.where((z == 1) & (k == 3), 0, lax.rem(k, 2))

    def streams(causal, later):
        hops = (z, 3 - z)
        to, back = (above, below), (below, above)

        def put(dir, u):
            slot = lax.rem(u, RING)
            return remote(sbuf.at[dir, lax.rem(u, SENDS)], ring.at[dir, slot], s_s.at[dir, lax.rem(u, SENDS)], s_r.at[dir, slot], to[dir])

        def emit(dir, u, value):
            def free():
                put(dir, u).wait_send()
            def credited():
                pl.semaphore_wait(credit.at[dir], 1)
            if later:
                free()
                credited()
            else:
                pl.when(u >= SENDS)(free)
                pl.when(u >= RING)(credited)
            sbuf[dir, lax.rem(u, SENDS)] = value().astype(BF16)
            put(dir, u).start()

        def one(dir, n):
            i = n - LAG * hops[dir]
            held = dir == 1 and causal
            if held:
                i = n - jnp.where(z == 0, HELD + LAG, LATE + LAG_DOWN * hops[dir])
            ic = jnp.maximum(i, 0)
            m, j = lax.div(ic, NT), lax.rem(ic, NT)
            if dir == 0:
                d, first_out, first_in = m + 1, NT * z, NT * (z - 1)
            elif causal:
                d, first_out, first_in = m, 0, 0
            else:
                d, first_out, first_in = 2 - m, NT * (3 - z), NT * (2 - z)
            on = (i >= 0) & (i < 3 * NT)
            beyond = (d > z) if dir == 0 else (d < z)
            u, v = jnp.maximum(i - first_out, 0), jnp.maximum(i - first_in, 0)
            has_in = hops[dir] > 0
            here = cols(j, T)

            def came():
                return ring[dir, lax.rem(v, RING)].astype(F32)

            @pl.when(on & beyond & (z != 1) if held else on & beyond)
            def _():
                @pl.when(has_in)
                def _():
                    put(dir, v).wait_recv()
                def value():
                    mine = pend[side_of(d, causal), :, here]
                    return jnp.where(has_in, mine + came(), mine)
                emit(dir, u, value)
                @pl.when(has_in)
                def _():
                    signal(credit.at[dir], back[dir])

            if held:
                @pl.when(on & beyond & (z == 1))
                def _():
                    put(dir, v).wait_recv()
                    pend[1, :, here] = pend[1, :, here] + came()
                    signal(credit.at[dir], back[dir])

                @pl.when((z == 1) & (n >= HELD) & (n < HELD + NT))
                def _():
                    u = n - HELD
                    emit(dir, u, lambda: pend[1, :, cols(u, T)])

            @pl.when(on & (d == z) & has_in)
            def _():
                put(dir, v).wait_recv()
                res[:, here] = res[:, here] + came()
                signal(credit.at[dir], back[dir])

        def step(n):
            for dir in range(2):
                one(dir, n)
            return 0

        def finish():
            for dir in range(2):
                @pl.when(hops[1 - dir] > 0)
                def _():
                    for n in range(SENDS):
                        put(dir, n).wait_send()
                    pl.semaphore_wait(credit.at[dir], RING)

        return step, finish

    def down(lhs, to_res, side, wait_free, weights, tile, stream, event):
        def send(s):
            return remote(sdb.at[lax.rem(s, 2)], d2buf.at[:, cols(s, 2 * T)], t_s.at[lax.rem(s, 2)], t_r.at[s], partner)

        def body(s, _):
            @pl.when(s >= 2)
            def _():
                send(s - 2).wait_recv()
                here = cols(s - 2, 2 * T)
                @pl.when(to_res)
                def _():
                    res[:, here] = res[:, here] + (st[lax.rem(s, 2)] + d2buf[:, here].astype(F32))
                @pl.when(jnp.logical_not(to_res))
                def _():
                    pend[side, :, here] = st[lax.rem(s, 2)] + d2buf[:, here].astype(F32)
            if stream is not None:
                @pl.when((s >= 2) & (lax.rem(s, 2) == 0))
                def _():
                    stream(lax.div(s, 2) - 1)
            if event is not None:
                @pl.when(s == 6)
                def _():
                    event()
            @pl.when(s < DOWN_STEPS)
            def _():
                weights(s)
                @pl.when(s >= 2)
                def _():
                    send(s - 2).wait_send()
                rows = lhs()
                for n in range(2):
                    got = _dot(rows, tile(s, n))
                    st[lax.rem(s, 2), :, n * T : (n + 1) * T] = got[:R]
                    sdb[lax.rem(s, 2), :, n * T : (n + 1) * T] = got[R:].astype(BF16)
                @pl.when((s == 0) & wait_free)
                def _():
                    pl.semaphore_wait(d2free, 1)
                send(s).start()
            return 0

        lax.fori_loop(0, DOWN_STEPS + 2, body, 0)
        for s in range(DOWN_STEPS - 2, DOWN_STEPS):
            send(s).wait_send()
        signal(d2free, partner)

    def normed(first, gain_ref):
        def body(i, _):
            rows = pl.ds(pl.multiple_of(i * 16, 16), 16)
            wide = xf[own, rows, :].astype(F32) if first else res[rows, :].astype(BF16).astype(F32)
            res[rows, :] = wide
            scale = lax.rsqrt(jnp.mean(wide * wide, -1, keepdims=True) + 1e-6)
            xf[own, rows, :] = (wide * scale * gain_ref[...].astype(F32)).astype(BF16)
            return 0
        lax.fori_loop(0, R // 16, body, 0)

    barrier = pltpu.get_barrier_semaphore()
    greet(barrier)
    load = pltpu.make_async_copy(x_ref, xf.at[own], ld_sem)
    load.start()
    for t in range(3):
        fetch_qkv(jnp.int32(t))
    load.wait()
    normed(True, ga_ref)
    pl.semaphore_wait(barrier, n_peers)
    start, event, events, landed, landed_own, end = gather(True)
    step, _ = streams(True, False)
    start()

    def tables(q):
        lane = lax.broadcasted_iota(jnp.int32, (C, HEAD), 1)
        place = (q * C + lax.broadcasted_iota(jnp.int32, (C, HEAD), 0)).astype(F32)
        low = lane < HEAD // 2
        power = -jnp.where(low, lane, lane - HEAD // 2).astype(F32) / (HEAD // 2)
        angle = place * jnp.exp(power * jnp.float32(LOG_THETA))
        cosb[...] = jnp.cos(angle)
        sinb[...] = jnp.where(low, -1.0, 1.0) * jnp.sin(angle)

    landed_own()

    mid = wbuf.at[2]

    def mid_rows(t, first, n):
        return pl.ds(pl.multiple_of(t * 1024 + first, R), n)

    def ready_at(k):
        need = jnp.where(z == 2, jnp.where(k == 1, 5, PIECES * k),
                         jnp.where(z == 3, jnp.where(k == 1, 6, jnp.where(k == 2, 9, PIECES * k)), PIECES * k))
        return jnp.minimum(need, 3 * PIECES)

    e = HEAD**-0.5 * LOG2E

    def attend(d):
        for i in range(8):
            @pl.when(d == i // 2)
            def _():
                n = R * (i + 1)

                def heads(h, _):
                    lane = pl.ds(pl.multiple_of(h * HEAD, HEAD), HEAD)
                    for th in range(2):
                        qr = mid_rows(th, R * i, R)
                        q = mid[qr, lane]
                        k = mid[mid_rows(2 + th, 0, n), lane]
                        v = mid[mid_rows(4 + th, 0, n), lane]
                        s = lax.dot_general(q, k, (((1,), (1,)), ((), ())), preferred_element_type=F32)
                        seen = lax.broadcasted_iota(jnp.int32, (R, R), 0) >= lax.broadcasted_iota(jnp.int32, (R, R), 1)
                        last = jnp.where(seen, s[:, n - R :], -1e30)
                        s = jnp.concatenate([s[:, : n - R], last], axis=1) if i else last
                        top = jnp.max(s, axis=1, keepdims=True)
                        p = jnp.exp2((s - top) * e).astype(BF16)
                        o = _dot(p, jnp.concatenate([v, jnp.ones((n, HEAD), BF16)], axis=1))
                        mid[qr, lane] = (o[:, :HEAD] / o[:, HEAD:]).astype(BF16)
                    return 0
                lax.fori_loop(0, 4, heads, 0)

    def out_lhs(d):
        def lhs():
            return jnp.concatenate([jnp.concatenate([mid[mid_rows(t, d * C + lane * R, R), :] for t in range(2)], axis=1)
                                    for lane in (c, 1 - c)], axis=0)
        return lhs

    def slot1(k, _):
        q = jnp.where(k == 0, z, jnp.where(k - 1 < z, k - 1, k))
        at, before = ready_at(k), ready_at(jnp.maximum(k - 1, 0))
        base = NT * (k - 2)

        @pl.when(k > 0)
        def _():
            for n in range(3):
                lax.fori_loop(0, 2, lambda i, _: step(base + 4 + 2 * n + i), 0)
                if n < 2:
                    @pl.when(before + 2 + n < at)
                    def _():
                        event(before + 2 + n)
            events(before + 4, at)
            landed(before, at)

        more = (k > 0) | (z == 0)
        tables(q)

        def qkv(t, _):
            @pl.when(lax.rem(t, 2) == 0)
            def _():
                step(base + 10 + lax.div(t, 2))
            @pl.when((t == jnp.where(k == 0, 6, jnp.where((k == 1) & (z == 2), 3, 9))) & (at < ready_at(k + 1)))
            def _():
                event(at)
            qkv_copy(t, wq).wait()
            @pl.when((t + 3 < QKV_STEPS) | jnp.logical_not(more))
            def _():
                fetch_qkv(lax.rem(t + 3, QKV_STEPS))
            @pl.when((t == 10) & more)
            def _():
                fetch_out(0)
            got = _dot(xf[pl.ds(2 * q, 2)].reshape(C, D), qkv_tile(t)[...]).astype(BF16).astype(F32)
            cos = jnp.where(t >= 8, 1.0, cosb[...])
            sin = jnp.where(t >= 8, 0.0, sinb[...])
            for n in range(2):
                part = got[:, n * HEAD : (n + 1) * HEAD]
                lane = pl.ds(pl.multiple_of(lax.rem(t, 2) * (W // 2) + n * HEAD, HEAD), HEAD)
                mid[mid_rows(lax.div(t, 2), q * C, C), lane] = (part * cos + pltpu.roll(part, HEAD // 2, 1) * sin).astype(BF16)
            return 0
        lax.fori_loop(0, QKV_STEPS, qkv, 0)

        @pl.when(more)
        def _():
            fetch_out(1)

        def second(now):
            @pl.when(now & (at + 1 < ready_at(k + 1)))
            def _():
                event(at + 1)
        second((z == 2) & (k == 1))

        def tile(s, n):
            a = 2 * s + n
            return wbuf[lax.div(a, 8), pl.ds(pl.multiple_of(lax.rem(a, 8) * 1024, 1024), 1024), :]

        def arrived(first):
            def weights(s):
                for half in range(2):
                    @pl.when((s == 4 * half) & first)
                    def _():
                        for copy in out_copies(half):
                            copy.wait()
            return weights

        @pl.when(k > 0)
        def _():
            attend(q)
            down(out_lhs(q), jnp.bool_(False), side_of(q, True), (k > 1) | (z == 0), arrived(jnp.bool_(True)), tile,
                 lambda n: step(NT * (k - 1) + n), None)

        @pl.when(k == z)
        def _():
            attend(z)
            down(out_lhs(z), jnp.bool_(True), 0, k > 0, arrived(k == 0), tile, None, None)

        @pl.when(more & (k < 3))
        def _():
            for t in range(3):
                fetch_qkv(jnp.int32(t))
        second((z != 2) | (k != 1))
        return 0

    lax.fori_loop(0, 4, slot1, 0)
    for t in range(2):
        fetch_gu(t, t)
    end()
    greet(ready)
    last = jnp.where(z == 2, LATE + LAG_DOWN, LAG * z)
    lax.fori_loop(2 * NT + 4, 3 * NT + last, lambda n, _: step(n), 0)

    normed(False, gm_ref)
    pl.semaphore_wait(ready, n_peers)
    start, event, events, landed, landed_own, end = gather(False)
    step2, finish = streams(False, True)
    start()
    landed_own()
    per = GU_STEPS + DOWN_STEPS

    def ahead2(g):
        r, slot = lax.rem(g + 2, per), lax.rem(g + 2, 3)
        @pl.when((g + 2 < 4 * per) & (r < GU_STEPS))
        def _():
            fetch_gu(r, slot)
        @pl.when((g + 2 < 4 * per) & (r >= GU_STEPS))
        def _():
            fetch_down(wd, r - GU_STEPS, slot)

    def slot2(k, _):
        low = jnp.where(k == 0, z, jnp.where(k - 1 < z, k - 1, k))
        zz = 3 - z
        high = 3 - jnp.where(k == 0, zz, jnp.where(k - 1 < zz, k - 1, k))
        q = jnp.where(z < 2, low, high)

        @pl.when(k > 0)
        def _():
            event(PIECES * k - 1)
            landed(PIECES * (k - 1), PIECES * k)

        def gu(t, _):
            g = per * k + t
            slot = lax.rem(g, 3)
            step2(NT * (k - 2) + 4 + t)
            @pl.when(((t == 5) | (t == 11)) & (k < 3))
            def _():
                event(PIECES * k + lax.div(t, 6))
            for copy in gu_copies(t, slot):
                copy.wait()
            ahead2(g)
            lhs = xf[pl.ds(2 * q, 2)].reshape(C, D)
            both = _dot(lhs, wbuf[slot])
            gate, up = both[:, : W // 2], both[:, W // 2 :]
            hid[:, :, cols(t, W // 2)] = (gate * jax.nn.sigmoid(gate) * up).astype(BF16).reshape(2, R, W // 2)
            return 0
        lax.fori_loop(0, GU_STEPS, gu, 0)

        def more():
            @pl.when(k < 3)
            def _():
                event(PIECES * k + 2)

        def weights(s):
            g = per * k + GU_STEPS + s
            for copy in down_copies(wd, s, lax.rem(g, 3)):
                copy.wait()
            ahead2(g)

        def tile(s, n):
            return wbuf[lax.rem(per * k + GU_STEPS + s, 3), n * HIDDEN : (n + 1) * HIDDEN, :]

        down(lambda: jnp.concatenate([hid[c], hid[1 - c]], axis=0), k == 0, side_of(q, False), jnp.bool_(True), weights, tile,
             lambda n: step2(NT * (k - 1) + n), more)
        return 0

    lax.fori_loop(0, 4, slot2, 0)
    end()
    lax.fori_loop(2 * NT + 4, 3 * NT + LAG * jnp.maximum(z, 3 - z), lambda n, _: step2(n), 0)

    def out(i, _):
        rows = pl.ds(pl.multiple_of(i * 16, 16), 16)
        xf[own, rows, :] = res[rows, :].astype(BF16)
        return 0
    lax.fori_loop(0, R // 16, out, 0)
    finish()
    pl.semaphore_wait(d2free, 1)
    store = pltpu.make_async_copy(xf.at[own], y_ref, ld_sem)
    store.start()
    store.wait()


def _layer(x, gain_a, wq, wk, wv, wo, gain_m, w_gate, w_up, w_down):
    hbm, vmem = pl.BlockSpec(memory_space=pl.ANY), pl.BlockSpec(memory_space=pltpu.VMEM)
    dma, regular = pltpu.SemaphoreType.DMA, pltpu.SemaphoreType.REGULAR
    n = 3 * PIECES
    return pl.pallas_call(
        _kernel,
        out_shape=jax.ShapeDtypeStruct((R, D), BF16),
        in_specs=[hbm, vmem, vmem] + [hbm] * 7,
        out_specs=hbm,
        scratch_shapes=[
            pltpu.VMEM((8, R, D), BF16),
            pltpu.VMEM((3, D, W), BF16),
            pltpu.VMEM((2, R, D), F32),
            pltpu.VMEM((R, D), F32),
            pltpu.VMEM((R, D), BF16),
            pltpu.VMEM((2, R, HIDDEN), BF16),
            pltpu.VMEM((2, R, 2 * T), F32),
            pltpu.VMEM((2, R, 2 * T), BF16),
            pltpu.VMEM((2, RING, R, T), BF16),
            pltpu.VMEM((2, SENDS, R, T), BF16),
            pltpu.VMEM((C, HEAD), F32),
            pltpu.VMEM((C, HEAD), F32),
            dma, dma((4,)),
            dma((2, n)), dma((2, n)), dma((2, n)), dma((2, n)), dma, dma,
            dma((2,)), dma((DOWN_STEPS,)), dma((2, SENDS)), dma((2, RING)),
            regular((2,)), regular, regular,
        ],
        compiler_params=pltpu.CompilerParams(collective_id=0, has_side_effects=True, vmem_limit_bytes=67043328),
    )(x, gain_a.reshape(1, D), gain_m.reshape(1, D), wq, wk, wv, wo, w_gate, w_up, w_down)


def solution(mesh):
    tokens, columns, rows_of = P(("dp", "tp"), None), P(None, "tp"), P("tp", None)
    return jax.shard_map(
        _layer,
        mesh=mesh,
        in_specs=(tokens, P(None), columns, columns, columns, rows_of, P(None), columns, columns, rows_of),
        out_specs=tokens,
        check_vma=False,
    )
```

```python
import functools

import jax
import jax.numpy as jnp
from jax import lax
from jax.experimental import pallas as pl
from jax.experimental.pallas import tpu as pltpu
from jax.sharding import PartitionSpec as P

HEAD = 128
LOG2E = 1.4426950408889634
LOG_THETA = 9.210340371976184
D = 8192
R = 128
C = 2 * R
PIECES = (8, 4)
W = 512
T = 512
NT = D // T
HIDDEN = 3072
QKV_STEPS, GU_STEPS, DOWN_STEPS = 12, 12, 8
RING, SENDS = 16, 4
UP_LAGS, DOWN_LAGS = ((0, 4, 6, 12), (0, 4, 2, 10)), ((32, 17, 8, 0), (14, 11, 3, 0))
HELD = 26
MESH = pl.DeviceIdType.MESH
F32, BF16 = jnp.float32, jnp.bfloat16
BOTH = (0, 1)
OWN = 2


def _half(n):
    return lax.div(n, 2)


def _odd(n):
    return lax.rem(n, 2)


def _dot(a, b):
    return jnp.dot(a, b, preferred_element_type=F32)


def _kernel(x_ref, ga_ref, gm_ref, wq, wk, wv, wo, wg, wu, wd, y_ref,
            xf, wbuf, pend, d2buf, hid, st, sdb, ring, sbuf,
            ld_sem, w_sem, ag_s, ag_r, gd_s, gd_r, own_s, own_r, t_s, t_r, s_s, s_r, credit, d2free, ready):
    dp, tp = lax.axis_index("dp"), lax.axis_index("tp")
    z, c = _half(tp), _odd(tp)
    up_z, down_z = jnp.minimum(z + 1, 3), jnp.maximum(z - 1, 0)
    partner, above, below = (dp, 2 * z + 1 - c), (dp, 2 * up_z + c), (dp, 2 * down_z + c)
    own = 2 * z + c
    res = pend.at[OWN]
    n_peers = 1 + jnp.minimum(z, 1) + jnp.minimum(3 - z, 1)

    def of_chip(values):
        return jnp.where(z == 0, values[0], jnp.where(z == 1, values[1], jnp.where(z == 2, values[2], values[3])))

    def remote(src, dst, send_sem, recv_sem, to):
        return pltpu.make_async_remote_copy(src, dst, send_sem, recv_sem, device_id=to, device_id_type=MESH)

    def signal(sem, to):
        pl.semaphore_signal(sem, inc=1, device_id=to, device_id_type=MESH)

    def greet(sem):
        signal(sem, partner)
        @pl.when(z < 3)
        def _():
            signal(sem, above)
        @pl.when(z > 0)
        def _():
            signal(sem, below)

    def cols(t, width):
        return pl.ds(pl.multiple_of(t * width, width), width)

    def qkv_tile(t):
        return wbuf.at[lax.rem(_half(t), 2), :, cols(_odd(t), W // 2)]

    def qkv_copy(t, w):
        return pltpu.make_async_copy(w.at[:, cols(lax.rem(t, 4), W // 2)], qkv_tile(t), w_sem.at[lax.rem(t, 4)])

    def fetch_qkv(t):
        for n, w in enumerate((wq, wk, wv)):
            @pl.when(lax.div(t, 4) == n)
            def _():
                qkv_copy(t, w).start()

    def out_copies(half):
        return [pltpu.make_async_copy(wo.at[:, (8 * half + n) * T : (8 * half + n + 1) * T], wbuf.at[half, n * 1024 : (n + 1) * 1024, :],
                                      w_sem.at[half]) for n in range(8)]

    def fetch_out(half):
        for copy in out_copies(half):
            copy.start()

    def gu_copies(t, slot):
        return [pltpu.make_async_copy(w.at[:, cols(t, W // 2)], wbuf.at[slot, :, pl.ds(n * (W // 2), W // 2)], w_sem.at[slot])
                for n, w in enumerate((wg, wu))]

    def fetch_gu(t, slot):
        for copy in gu_copies(t, slot):
            copy.start()

    def down_copies(w, s, slot):
        k = w.shape[0]
        return [pltpu.make_async_copy(w.at[:, cols(2 * s + n, W)], wbuf.at[slot, pl.ds(n * k, k), :], w_sem.at[slot]) for n in BOTH]

    def fetch_down(w, s, slot):
        for copy in down_copies(w, s, slot):
            copy.start()

    def gather(causal):
        pieces = PIECES[0 if causal else 1]
        size = R // pieces
        beats = (pieces * z, pieces * (3 - z))
        hop = (1 if causal else pieces, pieces)
        to = (above, below)
        can = (z < 3, z > 0)

        def place(dir, b):
            if dir == 1:
                chunk, piece = z + 1 + lax.div(b, pieces), lax.rem(b, pieces)
            elif not causal:
                chunk, piece = z - 1 - lax.div(b, pieces), lax.rem(b, pieces)
            else:
                o = b - (z - 1)
                later = jnp.maximum(o - pieces, 0)
                chunk = jnp.where(o < 0, z - 1 - b, jnp.where(o < pieces, 0, 1 + lax.div(later, pieces - 1)))
                piece = jnp.where(o < 0, 0, jnp.where(o < pieces, o, 1 + lax.rem(later, pieces - 1)))
            return chunk, pl.ds(pl.multiple_of(piece * size, size), size)

        def at(dir, b, lane):
            chunk, rows = place(dir, b)
            return xf.at[2 * chunk + lane, rows, :]

        def send(dir, ref, b):
            return remote(ref, ref, ag_s.at[dir, b], ag_r.at[dir, b], to[dir])

        def send_own(dir, piece, b):
            ref = xf.at[own, pl.ds(piece * size, size), :]
            @pl.when(can[dir])
            def _():
                send(dir, ref, b).start()

        def across(dir, b, lane):
            ref = at(dir, b, lane)
            return remote(ref, ref, gd_s.at[dir, b], gd_r.at[dir, b], partner)

        def across_own(lane):
            ref = xf.at[2 * z + lane]
            return remote(ref, ref, own_s, own_r, partner)

        def start():
            across_own(c).start()
            for piece in range(pieces):
                send_own(1, piece, piece)
                if not causal:
                    send_own(0, piece, piece)
            if causal:
                send_own(0, 0, 0)
                @pl.when(z == 0)
                def _():
                    for piece in range(1, pieces):
                        send_own(0, piece, piece)

        def numbered(dir, i):
            if causal:
                return i, i < beats[dir]
            near = (z == 1) if dir == 0 else (z == 2)
            far = (z == 2) if dir == 0 else (z == 1)
            alone = (z == 3) if dir == 0 else (z == 0)
            b = jnp.where(far, i - pieces, i)
            return b, alone | (near & (i < pieces)) | (far & (i >= pieces))

        def event(i):
            for dir in BOTH:
                b, some = numbered(dir, i)
                @pl.when(some)
                def _():
                    ref = at(dir, b, c)
                    send(dir, ref, b).wait_recv()
                    @pl.when(can[dir])
                    def _():
                        send(dir, ref, b + hop[dir]).start()
                    across(dir, b, c).start()
                    if dir == 0 and causal:
                        @pl.when(b == beats[0] - 1)
                        def _():
                            for piece in range(1, pieces):
                                send_own(0, piece, pieces * z + piece)

        def events(a, b):
            lax.fori_loop(a, b, lambda i, _: (event(i), 0)[1], 0)

        def landed(a, b):
            def body(i, _):
                for dir in BOTH:
                    b, some = numbered(dir, i)
                    @pl.when(some)
                    def _():
                        across(dir, b, 1 - c).wait_recv()
                return 0
            lax.fori_loop(a, b, body, 0)

        def landed_own():
            across_own(1 - c).wait_recv()

        def end():
            across_own(c).wait_send()
            for dir in BOTH:
                def sent(i, _):
                    send(dir, xf.at[own, pl.ds(0, size), :], i).wait_send()
                    return 0
                @pl.when(can[dir])
                def _():
                    lax.fori_loop(0, beats[dir] + pieces, sent, 0)
                def crossed(i, _):
                    across(dir, i, c).wait_send()
                    return 0
                lax.fori_loop(0, beats[dir], crossed, 0)

        return start, event, events, landed, landed_own, end

    def side_of(d, causal):
        if not causal:
            return jnp.where(d > z, 0, 1)
        k = jnp.where(d < z, d + 1, d)
        return jnp.where((z == 1) & (k == 3), 0, _odd(k))

    def streams(causal, later):
        hops = (z, 3 - z)
        half = 0 if causal else 1
        lags = (of_chip(UP_LAGS[half]), of_chip(DOWN_LAGS[half]))
        to, back = (above, below), (below, above)

        def put(dir, u):
            slot = lax.rem(u, RING)
            return remote(sbuf.at[dir, lax.rem(u, SENDS)], ring.at[dir, slot], s_s.at[dir, lax.rem(u, SENDS)], s_r.at[dir, slot], to[dir])

        def emit(dir, u, value):
            def free():
                put(dir, u).wait_send()
            def credited():
                pl.semaphore_wait(credit.at[dir], 1)
            if later:
                free()
                credited()
            else:
                pl.when(u >= SENDS)(free)
                pl.when(u >= RING)(credited)
            sbuf[dir, lax.rem(u, SENDS)] = value().astype(BF16)
            put(dir, u).start()

        def one(dir, n):
            i = n - lags[dir]
            held = dir == 1 and causal
            ic = jnp.maximum(i, 0)
            m, j = lax.div(ic, NT), lax.rem(ic, NT)
            if dir == 0:
                d, first_out, first_in = m + 1, NT * z, NT * (z - 1)
            elif causal:
                d, first_out, first_in = m, 0, 0
            else:
                d, first_out, first_in = 2 - m, NT * (3 - z), NT * (2 - z)
            on = (i >= 0) & (i < 3 * NT)
            beyond = (d > z) if dir == 0 else (d < z)
            u, v = jnp.maximum(i - first_out, 0), jnp.maximum(i - first_in, 0)
            has_in = hops[dir] > 0
            here = cols(j, T)

            def came():
                return ring[dir, lax.rem(v, RING)].astype(F32)

            @pl.when(on & beyond & (z != 1) if held else on & beyond)
            def _():
                @pl.when(has_in)
                def _():
                    put(dir, v).wait_recv()
                def value():
                    mine = pend[side_of(d, causal), :, here]
                    return jnp.where(has_in, mine + came(), mine)
                emit(dir, u, value)
                @pl.when(has_in)
                def _():
                    signal(credit.at[dir], back[dir])

            if held:
                @pl.when(on & beyond & (z == 1))
                def _():
                    put(dir, v).wait_recv()
                    pend[1, :, here] = pend[1, :, here] + came()
                    signal(credit.at[dir], back[dir])

                @pl.when((z == 1) & (n >= HELD) & (n < HELD + NT))
                def _():
                    u = n - HELD
                    emit(dir, u, lambda: pend[1, :, cols(u, T)])

            @pl.when(on & (d == z) & has_in)
            def _():
                put(dir, v).wait_recv()
                total = res[:, here] + came()
                res[:, here] = total
                signal(credit.at[dir], back[dir])
                if not causal:
                    @pl.when((z == 0) if dir == 1 else (z == 3))
                    def _():
                        xf[own, :, here] = total.astype(BF16)
                        pltpu.make_async_copy(xf.at[own, :, here], y_ref.at[:, here], ld_sem).start()

        def step(n):
            for dir in BOTH:
                one(dir, n)
            return 0

        def finish():
            for dir in BOTH:
                @pl.when(hops[1 - dir] > 0)
                def _():
                    for n in range(SENDS):
                        put(dir, n).wait_send()
                    pl.semaphore_wait(credit.at[dir], RING)

        return step, finish

    def down(lhs, side, wait_free, weights, tile, stream, event):
        def send(s):
            return remote(sdb.at[_odd(s)], d2buf.at[:, cols(s, 2 * T)], t_s.at[_odd(s)], t_r.at[s], partner)

        def body(s, dots, adds):
            before = s - 2
            if event is not None:
                event(s)
            if adds:
                send(before).wait_recv()
            if dots:
                weights(s)
                if adds:
                    send(before).wait_send()
            if adds:
                here = cols(before, 2 * T)
                term = st[_odd(s)] + d2buf[:, here].astype(F32)
                pend[side, :, here] = jnp.where(side == OWN, pend[side, :, here] + term, term)
            if dots:
                rows = lhs()
                for n in BOTH:
                    got = _dot(rows, tile(s, n))
                    st[_odd(s), :, n * T : (n + 1) * T] = got[:R]
                    sdb[_odd(s), :, n * T : (n + 1) * T] = got[R:].astype(BF16)
                if not adds:
                    @pl.when((s == 0) & wait_free)
                    def _():
                        pl.semaphore_wait(d2free, 1)
                send(s).start()
            if adds and stream is not None:
                stream(s)
            return 0

        lax.fori_loop(0, 2, lambda s, _: body(s, True, False), 0)
        lax.fori_loop(2, DOWN_STEPS, lambda s, _: body(s, True, True), 0)
        lax.fori_loop(DOWN_STEPS, DOWN_STEPS + 2, lambda s, _: body(s, False, True), 0)
        for s in range(DOWN_STEPS - 2, DOWN_STEPS):
            send(s).wait_send()
        signal(d2free, partner)

    def normed(first, gain_ref):
        def body(i, _):
            rows = pl.ds(pl.multiple_of(i * 16, 16), 16)
            wide = xf[own, rows, :].astype(F32) if first else res[rows, :].astype(BF16).astype(F32)
            res[rows, :] = wide
            scale = lax.rsqrt(jnp.mean(wide * wide, -1, keepdims=True) + 1e-6)
            xf[own, rows, :] = (wide * scale * gain_ref[...].reshape(1, D).astype(F32)).astype(BF16)
            return 0
        lax.fori_loop(0, R // 16, body, 0)

    barrier = pltpu.get_barrier_semaphore()
    greet(barrier)
    load = pltpu.make_async_copy(x_ref, xf.at[own], ld_sem)
    load.start()
    load.wait()
    for t in range(3):
        fetch_qkv(jnp.int32(t))
    normed(True, ga_ref)
    pl.semaphore_wait(barrier, n_peers)
    start, event, events, landed, landed_own, end = gather(True)
    step, _ = streams(True, False)
    start()

    def tables(q):
        lane = lax.broadcasted_iota(jnp.int32, (C, HEAD), 1)
        place = (q * C + lax.broadcasted_iota(jnp.int32, (C, HEAD), 0)).astype(F32)
        low = lane < HEAD // 2
        power = -jnp.where(low, lane, lane - HEAD // 2).astype(F32) / (HEAD // 2)
        angle = place * jnp.exp(power * jnp.float32(LOG_THETA))
        both = (jnp.cos(angle), jnp.where(low, -1.0, 1.0) * jnp.sin(angle))
        for n in BOTH:
            for lane in BOTH:
                st[n, :, lane * HEAD : (lane + 1) * HEAD] = both[n][lane * R : (lane + 1) * R]

    landed_own()

    mid = wbuf.at[2]

    def mid_rows(t, first, n):
        return pl.ds(pl.multiple_of(t * 1024 + first, R), n)

    def ready_at(k):
        first = PIECES[0]
        more = jnp.where(k == 1, jnp.maximum(z - 1, 0), jnp.where((k == 2) & (z == 3), 1, 0))
        return jnp.minimum(first * k + more, 3 * first)

    e = HEAD**-0.5 * LOG2E

    def attend(d):
        for i in range(8):
            @pl.when(d == i // 2)
            def _():
                n, many = R * (i + 1), 4 if i < 2 else 2 if i < 4 else 1

                def heads(h, _):
                    for th in range(2 * many):
                        lane = pl.ds(pl.multiple_of((h * many + th // 2) * HEAD, HEAD), HEAD)
                        th = th % 2
                        qr = mid_rows(th, R * i, R)
                        q = mid[qr, lane]
                        k = mid[mid_rows(2 + th, 0, n), lane]
                        v = mid[mid_rows(4 + th, 0, n), lane]
                        s = lax.dot_general(q, k, (((1,), (1,)), ((), ())), preferred_element_type=F32)
                        seen = lax.broadcasted_iota(jnp.int32, (R, R), 0) >= lax.broadcasted_iota(jnp.int32, (R, R), 1)
                        last = jnp.where(seen, s[:, n - R :], -1e30)
                        s = jnp.concatenate([s[:, : n - R], last], axis=1) if i else last
                        top = jnp.max(s, axis=1, keepdims=True)
                        p = jnp.exp2((s - top) * e).astype(BF16)
                        o = _dot(p, jnp.concatenate([v, jnp.ones((n, HEAD), BF16)], axis=1))
                        mid[qr, lane] = (o[:, :HEAD] / o[:, HEAD:]).astype(BF16)
                    return 0
                lax.fori_loop(0, 4 // many, heads, 0)

    def out_lhs(d):
        def lhs():
            return jnp.concatenate([jnp.concatenate([mid[mid_rows(t, d * C + lane * R, R), :] for t in BOTH], axis=1)
                                    for lane in (c, 1 - c)], axis=0)
        return lhs

    def slot1(k, _):
        q = jnp.where(k == 0, z, jnp.where(k - 1 < z, k - 1, k))
        at, before = ready_at(k), ready_at(k - 1) + jnp.where(k > 1, 5, 3)
        base = NT * (k - 2)

        @pl.when(k > 0)
        def _():
            for n in range(3):
                @pl.when((k == 1) | (k - 1 != z) if n < 2 else k >= 0)
                def _():
                    lax.fori_loop(0, 2, lambda i, _: step(base + 4 + 2 * n + i), 0)
                if n < 2:
                    @pl.when(before + n < at)
                    def _():
                        event(before + n)
            events(before + 2, at)
            landed(ready_at(k - 1), at)

        more = (k > 0) | (z == 0)
        tables(q)

        hurry = (z == 3) & (k == 1)

        def each_other(s, n):
            @pl.when((s >= 2) & (_odd(s) == 0))
            def _():
                step(n + _half(s) - 1)

        def further(n):
            @pl.when(at + n < ready_at(k + 1))
            def _():
                event(at + n)

        def qkv(t, _):
            @pl.when(_odd(t) == 0)
            def _():
                step(base + 10 + _half(t))
            @pl.when((lax.rem(t, 4) == 3) & jnp.logical_not(hurry))
            def _():
                further(lax.div(t, 4))
            qkv_copy(t, wq).wait()
            @pl.when((t + 3 < QKV_STEPS) | jnp.logical_not(more))
            def _():
                fetch_qkv(lax.rem(t + 3, QKV_STEPS))
            @pl.when((t == 10) & more)
            def _():
                fetch_out(0)
            got = _dot(xf[pl.ds(2 * q, 2)].reshape(C, D), qkv_tile(t)[...]).astype(BF16).astype(F32)
            cos, sin = [jnp.where(t >= 8, plain, jnp.concatenate([st[n, :, :HEAD], st[n, :, HEAD : 2 * HEAD]], axis=0))
                        for n, plain in enumerate((1.0, 0.0))]
            for n in BOTH:
                part = got[:, n * HEAD : (n + 1) * HEAD]
                lane = pl.ds(pl.multiple_of(_odd(t) * (W // 2) + n * HEAD, HEAD), HEAD)
                mid[mid_rows(_half(t), q * C, C), lane] = (part * cos + pltpu.roll(part, HEAD // 2, 1) * sin).astype(BF16)
            return 0
        lax.fori_loop(0, QKV_STEPS, qkv, 0)

        @pl.when(more)
        def _():
            fetch_out(1)

        def tile(s, n):
            a = 2 * s + n
            return wbuf[lax.div(a, 8), pl.ds(pl.multiple_of(lax.rem(a, 8) * 1024, 1024), 1024), :]

        def arrived(first):
            def weights(s):
                for half in BOTH:
                    @pl.when((s == 4 * half) & first)
                    def _():
                        for copy in out_copies(half):
                            copy.wait()
            return weights

        @pl.when(k > 0)
        def _():
            attend(q)
            further(3)
            down(out_lhs(q), side_of(q, True), (k > 1) | (z == 0), arrived(jnp.bool_(True)), tile,
                 lambda s: each_other(s, NT * (k - 1)), None)
            @pl.when(hurry)
            def _():
                for n in range(3):
                    further(n)
            further(4)

        @pl.when(k == z)
        def _():
            attend(z)
            down(out_lhs(z), jnp.int32(OWN), k > 0, arrived(k == 0), tile, lambda s: each_other(s, NT * (k - 1) + 4), None)

        @pl.when(more & (k < 3))
        def _():
            for t in range(3):
                fetch_qkv(jnp.int32(t))
        return 0

    lax.fori_loop(0, 4, slot1, 0)
    for t in BOTH:
        fetch_gu(t, t)
    end()
    greet(ready)
    last = of_chip((0, 4, 8, 12))
    lax.fori_loop(2 * NT + jnp.where(z == 3, 8, 4), 3 * NT + last, lambda n, _: step(n), 0)

    normed(False, gm_ref)
    pl.semaphore_wait(ready, n_peers)
    start, event, events, landed, landed_own, end = gather(False)
    step2, finish = streams(False, True)
    start()
    landed_own()
    per = GU_STEPS + DOWN_STEPS

    def ahead2(g):
        r, slot = lax.rem(g + 2, per), lax.rem(g + 2, 3)
        @pl.when((g + 2 < 4 * per) & (r < GU_STEPS))
        def _():
            fetch_gu(r, slot)
        @pl.when((g + 2 < 4 * per) & (r >= GU_STEPS))
        def _():
            fetch_down(wd, r - GU_STEPS, slot)

    def slot2(k, _):
        low = jnp.where(k == 0, z, jnp.where(k - 1 < z, k - 1, k))
        zz = 3 - z
        high = 3 - jnp.where(k == 0, zz, jnp.where(k - 1 < zz, k - 1, k))
        q = jnp.where(z < 2, low, high)
        inner = (z == 1) | (z == 2)

        @pl.when(k > 0)
        def _():
            @pl.when(jnp.logical_not(inner & (k > 1)))
            def _():
                event(PIECES[1] * k - 1)
            landed(PIECES[1] * (k - 1), PIECES[1] * k)

        def product(t):
            gate, up = st[:, :, : W // 2], st[:, :, W // 2 : W]
            hid[:, :, cols(t, W // 2)] = (gate * jax.nn.sigmoid(gate) * up).astype(BF16)

        def gu(t, _):
            g = per * k + t
            slot = lax.rem(g, 3)
            step2(NT * (k - 2) + 4 + t)
            early, late = inner & (k > 0), inner & (k == 0)
            now = (early & ((t == 0) | (t == 3) | (t == 7) | (t == 11))) | (late & ((t == 5) | (t == 11))) | (jnp.logical_not(inner) & (t == 11))
            @pl.when(now & (k < 3))
            def _():
                event(PIECES[1] * k + jnp.where(early, lax.div(t + 1, 4), jnp.where(late, lax.div(t, 6), 0)))
            for copy in gu_copies(t, slot):
                copy.wait()
            ahead2(g)
            product(jnp.maximum(t - 1, 0))
            st[:, :, :W] = _dot(xf[pl.ds(2 * q, 2)].reshape(C, D), wbuf[slot]).reshape(2, R, W)
            return 0

        lax.fori_loop(0, GU_STEPS, gu, 0)
        product(GU_STEPS - 1)

        @pl.when(k == 3)
        def _():
            end()

        def more(s):
            @pl.when((((s == 6) & jnp.logical_not(inner & (k > 0))) | ((s == 3) & jnp.logical_not(inner))) & (k < 3))
            def _():
                event(PIECES[1] * k + jnp.where(s == 3, 1, 2))

        def stream(s):
            @pl.when((k == 3) | (_odd(s) == 0))
            def _():
                step2(NT * (k - 1) + jnp.where(k == 3, s - 2, _half(s) - 1))

        def weights(s):
            g = per * k + GU_STEPS + s
            for copy in down_copies(wd, s, lax.rem(g, 3)):
                copy.wait()
            ahead2(g)

        def tile(s, n):
            return wbuf[lax.rem(per * k + GU_STEPS + s, 3), n * HIDDEN : (n + 1) * HIDDEN, :]

        down(lambda: jnp.concatenate([hid[c], hid[1 - c]], axis=0), jnp.where(k == 0, OWN, side_of(q, False)), jnp.bool_(True), weights, tile,
             stream, more)
        return 0

    lax.fori_loop(0, 4, slot2, 0)
    lax.fori_loop(2 * NT + 8, 3 * NT + of_chip((14, 11, 3, 10)), lambda n, _: step2(n), 0)

    store = pltpu.make_async_copy(xf.at[own], y_ref, ld_sem)

    @pl.when((z == 1) | (z == 2))
    def _():
        def out(i, _):
            rows = pl.ds(pl.multiple_of(i * 16, 16), 16)
            xf[own, rows, :] = res[rows, :].astype(BF16)
            return 0
        lax.fori_loop(0, R // 16, out, 0)
        store.start()
    finish()
    pl.semaphore_wait(d2free, 1)
    store.wait()


def _layer(x, gain_a, wq, wk, wv, wo, gain_m, w_gate, w_up, w_down):
    hbm, vmem = pl.BlockSpec(memory_space=pl.ANY), pl.BlockSpec(memory_space=pltpu.VMEM)
    dma, regular = pltpu.SemaphoreType.DMA, pltpu.SemaphoreType.REGULAR
    n = 3 * max(PIECES)
    return pl.pallas_call(
        _kernel,
        out_shape=jax.ShapeDtypeStruct((R, D), BF16),
        in_specs=[hbm, vmem, vmem] + [hbm] * 7,
        out_specs=hbm,
        scratch_shapes=[
            pltpu.VMEM((8, R, D), BF16),
            pltpu.VMEM((3, D, W), BF16),
            pltpu.VMEM((3, R, D), F32),
            pltpu.VMEM((R, D), BF16),
            pltpu.VMEM((2, R, HIDDEN), BF16),
            pltpu.VMEM((2, R, 2 * T), F32),
            pltpu.VMEM((2, R, 2 * T), BF16),
            pltpu.VMEM((2, RING, R, T), BF16),
            pltpu.VMEM((2, SENDS, R, T), BF16),
            dma, dma((4,)),
            dma((2, n)), dma((2, n)), dma((2, n)), dma((2, n)), dma, dma,
            dma((2,)), dma((DOWN_STEPS,)), dma((2, SENDS)), dma((2, RING)),
            regular((2,)), regular, regular,
        ],
        compiler_params=pltpu.CompilerParams(collective_id=0, has_side_effects=True, vmem_limit_bytes=67043328),
    )(x, gain_a, gain_m, wq, wk, wv, wo, w_gate, w_up, w_down)


def solution(mesh):
    tokens, columns, rows_of = P(("dp", "tp"), None), P(None, "tp"), P("tp", None)
    return jax.shard_map(
        _layer,
        mesh=mesh,
        in_specs=(tokens, P(None), columns, columns, columns, rows_of, P(None), columns, columns, rows_of),
        out_specs=tokens,
        check_vma=False,
    )
```

```python
import functools

import jax
import jax.numpy as jnp
from jax import lax
from jax.experimental import pallas as pl
from jax.experimental.pallas import tpu as pltpu
from jax.sharding import PartitionSpec as P

HEAD = 128
LOG2E = 1.4426950408889634
LOG_THETA = 9.210340371976184
D = 8192
R = 128
C = 2 * R
PIECES = (8, 4)
W = 512
T = 512
NT = D // T
HIDDEN = 3072
QKV_STEPS, GU_STEPS, DOWN_STEPS = 12, 12, 8
RING, SENDS = 16, 4
UP_LAGS, DOWN_LAGS = ((0, 4, 6, 12), (0, 5, 5, 12)), ((32, 17, 8, 0), (14, 12, 3, 0))
HELD = 26
MESH = pl.DeviceIdType.MESH
F32, BF16 = jnp.float32, jnp.bfloat16
BOTH = (0, 1)
SUB = 16
TOKENS = 1024
OWN = 2


def _half(n):
    return lax.div(n, 2)


def _odd(n):
    return lax.rem(n, 2)


def _dot(a, b):
    return jnp.dot(a, b, preferred_element_type=F32)


def _kernel(x_ref, ga_ref, gm_ref, wq, wk, wv, wo, wg, wu, wd, y_ref,
            xf, wbuf, pend, d2buf, hid, st, sdb, ring, sbuf,
            ld_sem, w_sem, ag_s, ag_r, gd_s, gd_r, own_s, own_r, t_s, t_r, s_s, s_r, credit, d2free, ready):
    dp, tp = lax.axis_index("dp"), lax.axis_index("tp")
    z, c = _half(tp), _odd(tp)
    up_z, down_z = jnp.minimum(z + 1, 3), jnp.maximum(z - 1, 0)
    partner, above, below = (dp, 2 * z + 1 - c), (dp, 2 * up_z + c), (dp, 2 * down_z + c)
    own = 2 * z + c
    res = pend.at[OWN]
    n_peers = 1 + jnp.minimum(z, 1) + jnp.minimum(3 - z, 1)

    def of_chip(values):
        return jnp.where(z == 0, values[0], jnp.where(z == 1, values[1], jnp.where(z == 2, values[2], values[3])))

    def remote(src, dst, send_sem, recv_sem, to):
        return pltpu.make_async_remote_copy(src, dst, send_sem, recv_sem, device_id=to, device_id_type=MESH)

    def signal(sem, to):
        pl.semaphore_signal(sem, inc=1, device_id=to, device_id_type=MESH)

    def greet(sem):
        signal(sem, partner)
        @pl.when(z < 3)
        def _():
            signal(sem, above)
        @pl.when(z > 0)
        def _():
            signal(sem, below)

    def cols(t, width):
        return pl.ds(pl.multiple_of(t * width, width), width)

    def qkv_tile(t):
        return wbuf.at[lax.rem(_half(t), 2), :, cols(_odd(t), W // 2)]

    def qkv_copy(t, w):
        return pltpu.make_async_copy(w.at[:, cols(lax.rem(t, 4), W // 2)], qkv_tile(t), w_sem.at[lax.rem(t, 4)])

    def fetch_qkv(t):
        for n, w in enumerate((wq, wk, wv)):
            @pl.when(lax.div(t, 4) == n)
            def _():
                qkv_copy(t, w).start()

    def out_copies(half):
        return [pltpu.make_async_copy(wo.at[:, (8 * half + n) * T : (8 * half + n + 1) * T], wbuf.at[half, n * TOKENS : (n + 1) * TOKENS, :],
                                      w_sem.at[half]) for n in range(8)]

    def fetch_out(half):
        for copy in out_copies(half):
            copy.start()

    def gu_copies(t, slot):
        return [pltpu.make_async_copy(w.at[:, cols(t, W // 2)], wbuf.at[slot, :, pl.ds(n * (W // 2), W // 2)], w_sem.at[slot])
                for n, w in enumerate((wg, wu))]

    def fetch_gu(t, slot):
        for copy in gu_copies(t, slot):
            copy.start()

    def down_copies(w, s, slot):
        k = w.shape[0]
        return [pltpu.make_async_copy(w.at[:, cols(2 * s + n, W)], wbuf.at[slot, pl.ds(n * k, k), :], w_sem.at[slot]) for n in BOTH]

    def fetch_down(w, s, slot):
        for copy in down_copies(w, s, slot):
            copy.start()

    def gather(causal):
        pieces = PIECES[0 if causal else 1]
        size = R // pieces
        beats = (pieces * z, pieces * (3 - z))
        hop = (1 if causal else pieces, pieces)
        to = (above, below)
        can = (z < 3, z > 0)

        def place(dir, b):
            if dir == 1:
                chunk, piece = z + 1 + lax.div(b, pieces), lax.rem(b, pieces)
            elif not causal:
                chunk, piece = z - 1 - lax.div(b, pieces), lax.rem(b, pieces)
            else:
                o = b - (z - 1)
                later = jnp.maximum(o - pieces, 0)
                chunk = jnp.where(o < 0, z - 1 - b, jnp.where(o < pieces, 0, 1 + lax.div(later, pieces - 1)))
                piece = jnp.where(o < 0, 0, jnp.where(o < pieces, o, 1 + lax.rem(later, pieces - 1)))
            return chunk, pl.ds(pl.multiple_of(piece * size, size), size)

        def at(dir, b, lane):
            chunk, rows = place(dir, b)
            return xf.at[2 * chunk + lane, rows, :]

        def send(dir, ref, b):
            return remote(ref, ref, ag_s.at[dir, b], ag_r.at[dir, b], to[dir])

        def send_own(dir, piece, b):
            ref = xf.at[own, pl.ds(pl.multiple_of(piece * size, size), size), :]
            @pl.when(can[dir])
            def _():
                send(dir, ref, b).start()

        def across(dir, b, lane):
            ref = at(dir, b, lane)
            return remote(ref, ref, gd_s.at[dir, b], gd_r.at[dir, b], partner)

        def across_own(lane, half):
            ref = xf.at[2 * z + lane, pl.ds(half * (R // 2), R // 2), :]
            return remote(ref, ref, own_s.at[half], own_r.at[half], partner)

        def leave(piece):
            send_own(1, piece, piece)
            if causal:
                @pl.when((piece == 0) | (z == 0))
                def _():
                    send_own(0, piece, piece)
            else:
                send_own(0, piece, piece)

        def start(norm):
            span = size // SUB

            def body(i, _):
                norm(i)
                @pl.when((i > 0) & (lax.rem(i, span) == 0))
                def _():
                    leave(lax.div(i, span) - 1)
                @pl.when(i == 5)
                def _():
                    across_own(c, 0).start()
                return 0
            lax.fori_loop(0, R // SUB, body, 0)
            leave(pieces - 1)
            across_own(c, 1).start()

        def numbered(dir, i):
            if causal:
                return i, i < beats[dir]
            near = (z == 1) if dir == 0 else (z == 2)
            far = (z == 2) if dir == 0 else (z == 1)
            alone = (z == 3) if dir == 0 else (z == 0)
            b = jnp.where(far, i - pieces, i)
            return b, alone | (near & (i < pieces)) | (far & (i >= pieces))

        def event(i):
            for dir in BOTH:
                b, some = numbered(dir, i)
                @pl.when(some)
                def _():
                    ref = at(dir, b, c)
                    send(dir, ref, b).wait_recv()
                    @pl.when(can[dir])
                    def _():
                        send(dir, ref, b + hop[dir]).start()
                    across(dir, b, c).start()
                    if dir == 0 and causal:
                        @pl.when(b == beats[0] - 1)
                        def _():
                            for piece in range(1, pieces):
                                send_own(0, piece, pieces * z + piece)

        def events(a, b):
            lax.fori_loop(a, b, lambda i, _: (event(i), 0)[1], 0)

        def landed(a, b):
            def body(i, _):
                for dir in BOTH:
                    b, some = numbered(dir, i)
                    @pl.when(some)
                    def _():
                        across(dir, b, 1 - c).wait_recv()
                return 0
            lax.fori_loop(a, b, body, 0)

        def landed_own():
            for half in BOTH:
                across_own(1 - c, half).wait_recv()

        def end():
            for half in BOTH:
                across_own(c, half).wait_send()
            for dir in BOTH:
                def sent(i, _):
                    send(dir, xf.at[own, pl.ds(0, size), :], i).wait_send()
                    return 0
                @pl.when(can[dir])
                def _():
                    lax.fori_loop(0, beats[dir] + pieces, sent, 0)
                def crossed(i, _):
                    across(dir, i, c).wait_send()
                    return 0
                lax.fori_loop(0, beats[dir], crossed, 0)

        return start, event, events, landed, landed_own, end

    def side_of(d, causal):
        if not causal:
            return jnp.where(d > z, 0, 1)
        k = jnp.where(d < z, d + 1, d)
        return jnp.where((z == 1) & (k == 3), 0, _odd(k))

    def streams(causal, later):
        hops = (z, 3 - z)
        half = 0 if causal else 1
        lags = (of_chip(UP_LAGS[half]), of_chip(DOWN_LAGS[half]))
        to, back = (above, below), (below, above)

        def put(dir, u):
            slot = lax.rem(u, RING)
            return remote(sbuf.at[dir, lax.rem(u, SENDS)], ring.at[dir, slot], s_s.at[dir, lax.rem(u, SENDS)], s_r.at[dir, slot], to[dir])

        def emit(dir, u, value):
            def free():
                put(dir, u).wait_send()
            def credited():
                pl.semaphore_wait(credit.at[dir], 1)
            if later:
                free()
                credited()
            else:
                pl.when(u >= SENDS)(free)
                pl.when(u >= RING)(credited)
            sbuf[dir, lax.rem(u, SENDS)] = value().astype(BF16)
            put(dir, u).start()

        def one(dir, n):
            i = n - lags[dir]
            held = dir == 1 and causal
            ic = jnp.maximum(i, 0)
            m, j = lax.div(ic, NT), lax.rem(ic, NT)
            if dir == 0:
                d, first_out, first_in = m + 1, NT * z, NT * (z - 1)
            elif causal:
                d, first_out, first_in = m, 0, 0
            else:
                d, first_out, first_in = 2 - m, NT * (3 - z), NT * (2 - z)
            on = (i >= 0) & (i < 3 * NT)
            beyond = (d > z) if dir == 0 else (d < z)
            u, v = jnp.maximum(i - first_out, 0), jnp.maximum(i - first_in, 0)
            has_in = hops[dir] > 0
            here = cols(j, T)

            def came():
                return ring[dir, lax.rem(v, RING)].astype(F32)

            @pl.when(on & beyond & (z != 1) if held else on & beyond)
            def _():
                @pl.when(has_in)
                def _():
                    put(dir, v).wait_recv()
                def value():
                    mine = pend[side_of(d, causal), :, here]
                    return jnp.where(has_in, mine + came(), mine)
                emit(dir, u, value)
                @pl.when(has_in)
                def _():
                    signal(credit.at[dir], back[dir])

            if held:
                @pl.when(on & beyond & (z == 1))
                def _():
                    put(dir, v).wait_recv()
                    pend[1, :, here] = pend[1, :, here] + came()
                    signal(credit.at[dir], back[dir])

                @pl.when((z == 1) & (n >= HELD) & (n < HELD + NT))
                def _():
                    u = n - HELD
                    emit(dir, u, lambda: pend[1, :, cols(u, T)])

            @pl.when(on & (d == z) & has_in)
            def _():
                put(dir, v).wait_recv()
                total = res[:, here] + came()
                res[:, here] = total
                signal(credit.at[dir], back[dir])
                if not causal:
                    @pl.when((z == 0) if dir == 1 else (z == 3))
                    def _():
                        xf[own, :, here] = total.astype(BF16)
                        pltpu.make_async_copy(xf.at[own, :, here], y_ref.at[:, here], ld_sem).start()

        def step(n, ahead=0):
            for dir in BOTH:
                one(dir, n + (ahead if dir == 0 else 0))
            return 0

        def finish():
            for dir in BOTH:
                @pl.when(hops[1 - dir] > 0)
                def _():
                    for n in range(SENDS):
                        put(dir, n).wait_send()
                    pl.semaphore_wait(credit.at[dir], RING)

        return step, one, finish

    def down(lhs, side, wait_free, weights, tile, stream, event):
        def send(s):
            return remote(sdb.at[_odd(s)], d2buf.at[:, cols(s, 2 * T)], t_s.at[_odd(s)], t_r.at[s], partner)

        def body(s, dots, adds):
            before = s - 2
            if event is not None:
                event(s)
            if adds:
                send(before).wait_recv()
            if dots:
                weights(s)
                if adds:
                    send(before).wait_send()
            if adds:
                here = cols(before, 2 * T)
                term = st[_odd(s)] + d2buf[:, here].astype(F32)
                pend[side, :, here] = jnp.where(side == OWN, pend[side, :, here] + term, term)
            if dots:
                rows = lhs()
                for n in BOTH:
                    got = _dot(rows, tile(s, n))
                    st[_odd(s), :, n * T : (n + 1) * T] = got[:R]
                    sdb[_odd(s), :, n * T : (n + 1) * T] = got[R:].astype(BF16)
                if not adds:
                    @pl.when((s == 0) & wait_free)
                    def _():
                        pl.semaphore_wait(d2free, 1)
                send(s).start()
            if adds and stream is not None:
                stream(s)
            return 0

        lax.fori_loop(0, 2, lambda s, _: body(s, True, False), 0)
        lax.fori_loop(2, DOWN_STEPS, lambda s, _: body(s, True, True), 0)
        lax.fori_loop(DOWN_STEPS, DOWN_STEPS + 2, lambda s, _: body(s, False, True), 0)
        for s in range(DOWN_STEPS - 2, DOWN_STEPS):
            send(s).wait_send()
        signal(d2free, partner)

    def normed(first, gain_ref):
        def body(i):
            rows = pl.ds(pl.multiple_of(i * SUB, SUB), SUB)
            wide = xf[own, rows, :].astype(F32) if first else res[rows, :].astype(BF16).astype(F32)
            res[rows, :] = wide
            scale = lax.rsqrt(jnp.mean(wide * wide, -1, keepdims=True) + 1e-6)
            xf[own, rows, :] = (wide * scale * gain_ref[...].reshape(1, D).astype(F32)).astype(BF16)
        return body

    barrier = pltpu.get_barrier_semaphore()
    greet(barrier)
    load = pltpu.make_async_copy(x_ref, xf.at[own], ld_sem)
    load.start()
    load.wait()
    for t in range(3):
        fetch_qkv(jnp.int32(t))
    pl.semaphore_wait(barrier, n_peers)
    start, event, events, landed, landed_own, end = gather(True)
    step, one, _ = streams(True, False)
    start(normed(True, ga_ref))

    def tables(q):
        lane = lax.broadcasted_iota(jnp.int32, (C, HEAD), 1)
        place = (q * C + lax.broadcasted_iota(jnp.int32, (C, HEAD), 0)).astype(F32)
        low = lane < HEAD // 2
        power = -jnp.where(low, lane, lane - HEAD // 2).astype(F32) / (HEAD // 2)
        angle = place * jnp.exp(power * jnp.float32(LOG_THETA))
        both = (jnp.cos(angle), jnp.where(low, -1.0, 1.0) * jnp.sin(angle))
        for n in BOTH:
            for lane in BOTH:
                st[n, :, lane * HEAD : (lane + 1) * HEAD] = both[n][lane * R : (lane + 1) * R]

    landed_own()

    mid = wbuf.at[2]

    def mid_rows(t, first, n):
        return pl.ds(pl.multiple_of(t * TOKENS + first, R), n)

    def ready_at(k):
        first = PIECES[0]
        more = jnp.where(k == 1, jnp.maximum(z - 1, 0), jnp.where((k == 2) & (z == 3), 1, 0))
        return jnp.minimum(first * k + more, 3 * first)

    e = HEAD**-0.5 * LOG2E

    def attend(d):
        for i in range(8):
            @pl.when(d == i // 2)
            def _():
                n, many = R * (i + 1), 4 if i < 3 else 2 if i < 6 else 1

                def heads(h, _):
                    for th in range(2 * many):
                        lane = pl.ds(pl.multiple_of((h * many + th // 2) * HEAD, HEAD), HEAD)
                        th = th % 2
                        qr = mid_rows(th, R * i, R)
                        q = mid[qr, lane]
                        k = mid[mid_rows(2 + th, 0, n), lane]
                        v = mid[mid_rows(4 + th, 0, n), lane]
                        s = lax.dot_general(q, k, (((1,), (1,)), ((), ())), preferred_element_type=F32)
                        seen = lax.broadcasted_iota(jnp.int32, (R, R), 0) >= lax.broadcasted_iota(jnp.int32, (R, R), 1)
                        last = jnp.where(seen, s[:, n - R :], -1e30)
                        s = jnp.concatenate([s[:, : n - R], last], axis=1) if i else last
                        top = jnp.max(s, axis=1, keepdims=True)
                        p = jnp.exp2((s - top) * e).astype(BF16)
                        o = _dot(p, jnp.concatenate([v, jnp.ones((n, HEAD), BF16)], axis=1))
                        mid[qr, lane] = (o[:, :HEAD] / o[:, HEAD:]).astype(BF16)
                    return 0
                lax.fori_loop(0, 4 // many, heads, 0)

    def out_lhs(d):
        def lhs():
            return jnp.concatenate([jnp.concatenate([mid[mid_rows(t, d * C + lane * R, R), :] for t in BOTH], axis=1)
                                    for lane in (c, 1 - c)], axis=0)
        return lhs

    def slot1(k, _):
        q = jnp.where(k == 0, z, jnp.where(k - 1 < z, k - 1, k))
        at, before = ready_at(k), ready_at(k - 1) + jnp.where(k > 1, 5, 3)
        base = NT * (k - 2)
        tables(q)

        @pl.when(k > 0)
        def _():
            for n in range(3):
                @pl.when((k == 1) | (k - 1 != z) if n < 2 else k >= 0)
                def _():
                    lax.fori_loop(0, 2, lambda i, _: step(base + 4 + 2 * n + i), 0)
                if n < 2:
                    @pl.when(before + n < at)
                    def _():
                        event(before + n)
            events(before + 2, at)
            landed(ready_at(k - 1), at)

        more = (k > 0) | (z == 0)

        ends = (z == 0) | (z == 3)
        hurry = ends & (k == 1)

        def each_other(s, n):
            @pl.when((s >= 2) & (_odd(s) == 0))
            def _():
                step(n + _half(s) - 1)

        def further(n):
            @pl.when(at + n < ready_at(k + 1))
            def _():
                event(at + n)

        def qkv(t, _):
            @pl.when(_odd(t) == 0)
            def _():
                step(base + 10 + _half(t))
            @pl.when((lax.rem(t, 4) == 3) & jnp.logical_not(hurry))
            def _():
                further(lax.div(t, 4))
            qkv_copy(t, wq).wait()
            @pl.when((t + 3 < QKV_STEPS) | jnp.logical_not(more))
            def _():
                fetch_qkv(lax.rem(t + 3, QKV_STEPS))
            @pl.when((t == 10) & more)
            def _():
                fetch_out(0)
            got = _dot(xf[pl.ds(2 * q, 2)].reshape(C, D), qkv_tile(t)[...]).astype(BF16).astype(F32)
            cos, sin = [jnp.where(t >= 8, plain, jnp.concatenate([st[n, :, :HEAD], st[n, :, HEAD : 2 * HEAD]], axis=0))
                        for n, plain in enumerate((1.0, 0.0))]
            for n in BOTH:
                part = got[:, n * HEAD : (n + 1) * HEAD]
                lane = pl.ds(pl.multiple_of(_odd(t) * (W // 2) + n * HEAD, HEAD), HEAD)
                mid[mid_rows(_half(t), q * C, C), lane] = (part * cos + pltpu.roll(part, HEAD // 2, 1) * sin).astype(BF16)
            return 0
        lax.fori_loop(0, QKV_STEPS, qkv, 0)

        @pl.when(more)
        def _():
            fetch_out(1)

        def tile(s, n):
            a = 2 * s + n
            return wbuf[lax.div(a, 8), pl.ds(pl.multiple_of(lax.rem(a, 8) * TOKENS, TOKENS), TOKENS), :]

        def arrived(first):
            def weights(s):
                for half in BOTH:
                    @pl.when((s == 4 * half) & first)
                    def _():
                        for copy in out_copies(half):
                            copy.wait()
            return weights

        @pl.when(k > 0)
        def _():
            attend(q)
            @pl.when(jnp.logical_not(ends & (k == 1)))
            def _():
                further(3)
            down(out_lhs(q), side_of(q, True), (k > 1) | (z == 0), arrived(jnp.bool_(True)), tile,
                 lambda s: each_other(s, NT * (k - 1)), None)
            @pl.when(hurry)
            def _():
                for n in range(3):
                    further(n)
            @pl.when(ends & (k == 1))
            def _():
                further(3)
            further(4)

        @pl.when(k == z)
        def _():
            attend(z)
            down(out_lhs(z), jnp.int32(OWN), k > 0, arrived(k == 0), tile, lambda s: each_other(s, NT * (k - 1) + 4), None)

        @pl.when(more & (k < 3))
        def _():
            for t in range(3):
                fetch_qkv(jnp.int32(t))
        return 0

    lax.fori_loop(0, 4, slot1, 0)
    for t in BOTH:
        fetch_gu(t, t)
    end()
    greet(ready)
    last = of_chip((0, 4, 8, 12))
    first, ahead = 2 * NT + jnp.where(z == 3, 8, 4), jnp.where(z == 2, 3, 0)
    lax.fori_loop(first, first + ahead, lambda n, _: (one(0, n), 0)[1], 0)
    lax.fori_loop(first, 3 * NT + last, lambda n, _: step(n, ahead), 0)

    pl.semaphore_wait(ready, n_peers)
    start, event, events, landed, landed_own, end = gather(False)
    step2, _, finish = streams(False, True)
    start(normed(False, gm_ref))
    landed_own()
    per = GU_STEPS + DOWN_STEPS

    def ahead2(g):
        r, slot = lax.rem(g + 2, per), lax.rem(g + 2, 3)
        @pl.when((g + 2 < 4 * per) & (r < GU_STEPS))
        def _():
            fetch_gu(r, slot)
        @pl.when((g + 2 < 4 * per) & (r >= GU_STEPS))
        def _():
            fetch_down(wd, r - GU_STEPS, slot)

    def slot2(k, _):
        low = jnp.where(k == 0, z, jnp.where(k - 1 < z, k - 1, k))
        zz = 3 - z
        high = 3 - jnp.where(k == 0, zz, jnp.where(k - 1 < zz, k - 1, k))
        q = jnp.where(z < 2, low, high)
        inner = (z == 1) | (z == 2)

        @pl.when(k > 0)
        def _():
            @pl.when(jnp.logical_not(inner & (k > 1)))
            def _():
                event(PIECES[1] * k - 1)
            landed(PIECES[1] * (k - 1), PIECES[1] * k)

        def product(t):
            gate, up = st[:, :, : W // 2], st[:, :, W // 2 : W]
            hid[:, :, cols(t, W // 2)] = (gate * jax.nn.sigmoid(gate) * up).astype(BF16)

        def gu(t, _):
            g = per * k + t
            slot = lax.rem(g, 3)
            step2(NT * (k - 2) + 4 + t)
            early, late = inner & (k > 0), inner & (k == 0)
            now = (early & ((t == 0) | (t == 3) | (t == 7) | (t == 11))) | (late & ((t == 5) | (t == 11))) | (jnp.logical_not(inner) & (t == 11))
            @pl.when(now & (k < 3))
            def _():
                event(PIECES[1] * k + jnp.where(early, lax.div(t + 1, 4), jnp.where(late, lax.div(t, 6), 0)))
            for copy in gu_copies(t, slot):
                copy.wait()
            ahead2(g)
            product(jnp.maximum(t - 1, 0))
            st[:, :, :W] = _dot(xf[pl.ds(2 * q, 2)].reshape(C, D), wbuf[slot]).reshape(2, R, W)
            return 0

        lax.fori_loop(0, GU_STEPS, gu, 0)
        product(GU_STEPS - 1)

        @pl.when(k == 3)
        def _():
            end()

        def more(s):
            @pl.when((((s == 6) & jnp.logical_not(inner & (k > 0))) | ((s == 3) & jnp.logical_not(inner))) & (k < 3))
            def _():
                event(PIECES[1] * k + jnp.where(s == 3, 1, 2))

        def stream(s):
            @pl.when((k == 3) | (_odd(s) == 0))
            def _():
                step2(NT * (k - 1) + jnp.where(k == 3, s - 2, _half(s) - 1))

        def weights(s):
            g = per * k + GU_STEPS + s
            for copy in down_copies(wd, s, lax.rem(g, 3)):
                copy.wait()
            ahead2(g)

        def tile(s, n):
            return wbuf[lax.rem(per * k + GU_STEPS + s, 3), n * HIDDEN : (n + 1) * HIDDEN, :]

        down(lambda: jnp.concatenate([hid[c], hid[1 - c]], axis=0), jnp.where(k == 0, OWN, side_of(q, False)), jnp.bool_(True), weights, tile,
             stream, more)
        return 0

    lax.fori_loop(0, 4, slot2, 0)
    lax.fori_loop(2 * NT + 8, 3 * NT + of_chip((14, 12, 5, 12)), lambda n, _: step2(n), 0)

    store = pltpu.make_async_copy(xf.at[own], y_ref, ld_sem)

    @pl.when((z == 1) | (z == 2))
    def _():
        def out(i, _):
            rows = pl.ds(pl.multiple_of(i * SUB, SUB), SUB)
            xf[own, rows, :] = res[rows, :].astype(BF16)
            return 0
        lax.fori_loop(0, R // SUB, out, 0)
        store.start()
    finish()
    pl.semaphore_wait(d2free, 1)
    store.wait()


def _layer(x, gain_a, wq, wk, wv, wo, gain_m, w_gate, w_up, w_down):
    hbm, vmem = pl.BlockSpec(memory_space=pl.ANY), pl.BlockSpec(memory_space=pltpu.VMEM)
    dma, regular = pltpu.SemaphoreType.DMA, pltpu.SemaphoreType.REGULAR
    n = 3 * max(PIECES)
    return pl.pallas_call(
        _kernel,
        out_shape=jax.ShapeDtypeStruct((R, D), BF16),
        in_specs=[hbm, vmem, vmem] + [hbm] * 7,
        out_specs=hbm,
        scratch_shapes=[
            pltpu.VMEM((8, R, D), BF16),
            pltpu.VMEM((3, D, W), BF16),
            pltpu.VMEM((3, R, D), F32),
            pltpu.VMEM((R, D), BF16),
            pltpu.VMEM((2, R, HIDDEN), BF16),
            pltpu.VMEM((2, R, 2 * T), F32),
            pltpu.VMEM((2, R, 2 * T), BF16),
            pltpu.VMEM((2, RING, R, T), BF16),
            pltpu.VMEM((2, SENDS, R, T), BF16),
            dma, dma((4,)),
            dma((2, n)), dma((2, n)), dma((2, n)), dma((2, n)), dma((2,)), dma((2,)),
            dma((2,)), dma((DOWN_STEPS,)), dma((2, SENDS)), dma((2, RING)),
            regular((2,)), regular, regular,
        ],
        compiler_params=pltpu.CompilerParams(collective_id=0, has_side_effects=True, vmem_limit_bytes=67043328),
    )(x, gain_a, gain_m, wq, wk, wv, wo, w_gate, w_up, w_down)


def solution(mesh):
    tokens, columns, rows_of = P(("dp", "tp"), None), P(None, "tp"), P("tp", None)
    return jax.shard_map(
        _layer,
        mesh=mesh,
        in_specs=(tokens, P(None), columns, columns, columns, rows_of, P(None), columns, columns, rows_of),
        out_specs=tokens,
        check_vma=False,
    )
```
